256 devices in a mesh: orb: 32 (over y_lo, z, core), slab: 8 (over y_hi, x).
Axes of the slice: x: 4, y: 4 (y_hi: 2, y_lo: 2; y = y_hi * 2 + y_lo), z: 8, core: 2. Of those that a mesh axis runs over, the one named last changes fastest.
Arguments:
- orbitals: bfloat16 [512, 32768], P('orb', 'slab'), may hold values from -6 to 6
- eigenpotentials: bfloat16 [1024, 32768], P(None, 'slab'), may hold values from -0.03125 to 0.03125
- screening: float32 [1024], replicated, may hold values from 0.02 to 2
- trial_vectors: bfloat16 [16, 32768], P(None, 'orb'), may hold values from -0.001953125 to 0.001953125
- pair_index: int32 [2, 32768], P(None, 'orb'), may hold values from -1 to 511, as said below
Outputs:
- direct: float32 [16, 32768], P(None, 'orb')
The draws below stay inside these ranges and needn't reach their ends.
Inputs may be any that keep to these rules, and one draw needn't show every extreme that they name: `pair_index`: each column is a pair (i, j) of two different orbitals, or holds -1 in both rows for an empty slot. The 1024 slots of one pair owner (one device of orb) hold its pairs; in every draw some owner has all of its slots used.
All inputs are finite; a program needn't handle non-finite values.
Results may differ from the reference program's by a relative error of at most 0.0091.
Values may be sent and summed in bfloat16 or wider, within the bound.
No kernel may reach another device: no remote copies, remote signals or barrier semaphores. Data moves between devices by JAX's collectives and lax.ppermute only.
A program may use at most 128 MiB of HBM per device.

```python
import math
import jax
import jax.numpy as jnp
from jax import lax

ORBS = 512
NEIG = 1024
NB = 16
P_DEV = 1024
NGRID = 32768
PAIRS = 32768


def draw_pair_index(key, part):
    owners = PAIRS // P_DEV
    keys = jax.random.split(jax.random.fold_in(key, 17), 6)
    counts = jax.random.randint(keys[0], (owners,), P_DEV // 4, P_DEV // 2 + 1)
    full_owner = jax.random.randint(keys[1], (), 0, owners)
    counts = jnp.where(jnp.arange(owners) == full_owner, P_DEV, counts)
    left_draw = jax.random.randint(keys[2], (PAIRS,), 0, ORBS)
    right_draw = jax.random.randint(keys[3], (PAIRS,), 0, ORBS)
    shuffle_table = jax.random.permutation(keys[4], ORBS).astype(jnp.int32)
    first_orbital = jnp.take(shuffle_table, left_draw * right_draw // ORBS)
    offsets = jax.random.randint(keys[5], (PAIRS,), 1, ORBS)
    second_orbital = (first_orbital + offsets) % ORBS
    slots = jnp.arange(PAIRS) % P_DEV
    owner_ids = jnp.arange(PAIRS) // P_DEV
    is_live = slots < jnp.take(counts, owner_ids)
    first_orbital = jnp.where(is_live, first_orbital, -1)
    second_orbital = jnp.where(is_live, second_orbital, -1)
    return jnp.stack([first_orbital, second_orbital]).astype(jnp.int32)


def block_scale(key, extent, shards, least, high):
    def one(axis_at, blocks):
        draws = jax.random.uniform(jax.random.fold_in(jax.random.fold_in(key, 6), axis_at), (blocks,), jnp.float32, least / len(shards), high / len(shards))
        return jnp.repeat(jnp.exp(draws), extent[axis_at] // blocks).reshape((-1,) + (1,) * (len(extent) - axis_at - 1))

    loudness = one(*shards[0])
    for cut in shards[1:]:
        loudness = loudness * one(*cut)
    return loudness


def gaussian(rng, dims, scale, most, shards=(), dtype=jnp.bfloat16):
    loudness = block_scale(rng, dims, shards, -0.22, 0.18) if shards else 1.0
    values = jax.random.normal(rng, dims, jnp.float32) * scale * loudness
    return jnp.minimum(jnp.maximum(values, -most), most).astype(dtype)


def setup_inputs(seed: int = 0) -> dict:
    streams_of = jax.random.split(jax.random.key(seed), 6)
    orbitals = gaussian(streams_of[0], (ORBS, NGRID), 1.0, 6.0, ((0, 32), (1, 8)))
    eigenpotentials = gaussian(streams_of[1], (NEIG, NGRID), NGRID ** -0.5, 0.03125, ((1, 8),))
    screening = jnp.clip(jnp.exp(jax.random.uniform(streams_of[2], (NEIG,), jnp.float32, math.log(0.02), math.log(2.0))), 0.02, 2.0)
    trial_vectors = gaussian(streams_of[3], (NB, PAIRS), (PAIRS * NEIG // 4) ** -0.5, 0.001953125, ((1, 32),))
    pair_index = draw_pair_index(jax.random.fold_in(streams_of[5], 71), 0)
    return {"orbitals": orbitals, "eigenpotentials": eigenpotentials, "screening": screening, "trial_vectors": trial_vectors, "pair_index": pair_index}


def block_density(orbitals, index_block):
    is_live = index_block[0] >= 0
    first_rows = jnp.take(orbitals, jnp.maximum(index_block[0], 0).astype(jnp.int32), axis=0).astype(jnp.float32)
    second_rows = jnp.take(orbitals, jnp.maximum(index_block[1], 0).astype(jnp.int32), axis=0).astype(jnp.float32)
    product = jnp.where(is_live[:, None], first_rows * second_rows, jnp.zeros((), jnp.float32))
    return product.astype(jnp.bfloat16)


def reference(orbitals, eigenpotentials, screening, trial_vectors, pair_index):
    blocks = PAIRS // P_DEV
    index_blocks = pair_index.reshape(2, blocks, P_DEV).transpose(1, 0, 2)
    trial_blocks = trial_vectors.reshape(NB, blocks, P_DEV).transpose(1, 0, 2)
    potentials = eigenpotentials.astype(jnp.float32)

    def accumulate(carry, item):
        index_block, trial_block = item
        density = block_density(orbitals, index_block).astype(jnp.float32)
        term = jnp.dot(trial_block.astype(jnp.float32), density, precision=lax.Precision.HIGHEST)
        return carry + term, None

    field_sum, unused = lax.scan(accumulate, jnp.zeros((NB, NGRID), jnp.float32), (index_blocks, trial_blocks))
    projected = lax.dot_general(field_sum, potentials, (((1,), (1,)), ((), ())), precision=lax.Precision.HIGHEST)
    screened = projected * screening.astype(jnp.float32)[None, :]
    potential = jnp.dot(screened, potentials, precision=lax.Precision.HIGHEST)

    def apply_block(index_block):
        density = block_density(orbitals, index_block).astype(jnp.float32)
        return lax.dot_general(potential, density, (((1,), (1,)), ((), ())), precision=lax.Precision.HIGHEST)

    direct_blocks = lax.map(apply_block, index_blocks)
    return direct_blocks.transpose(1, 0, 2).reshape(NB, PAIRS)
```

```python
import jax
import jax.numpy as jnp
from jax import lax
from jax.experimental import pallas as pl
from jax.experimental.pallas import tpu as pltpu
from jax.sharding import Mesh, PartitionSpec as P

AXES = ("yl", "zh", "zl", "c", "yh", "x")
SIZES = (2, 4, 2, 2, 2, 4)
ORB = ("yl", "zh", "zl", "c")
SLAB = ("yh", "x")
GROUP = ("yl", "zl", "c")
COLUMN = ("zh", "zl", "c")
PLANE = ("yl", "yh", "x")

f32 = jnp.float32
bf16 = jnp.bfloat16


def exchange(blocks, axes):
    return lax.all_to_all(blocks, axes, 0, 0, tiled=True)


def summed(blocks):
    return jnp.sum(blocks.astype(f32), axis=0)


def copies(value, count):
    return jnp.broadcast_to(value[None], (count, *value.shape))


def in_two(value):
    upper = value.astype(bf16)
    lower = (value - upper.astype(f32)).astype(bf16)
    return jnp.concatenate([upper, lower], axis=0)


def dot(left, right, dims=(((1,), (0,)), ((), ()))):
    return lax.dot_general(left, right, dims, preferred_element_type=f32)


NT = (((1,), (1,)), ((), ()))


def density_body(where_ref, phi_ref, slots_ref, pot_ref, dens_ref, proj_ref, phit_ref, fieldt_ref):
    step = pl.program_id(0)

    @pl.when(step == 0)
    def _():
        phit_ref[...] = phi_ref[...].T
        fieldt_ref[...] = jnp.zeros_like(fieldt_ref)

    slots = slots_ref[0]
    width = slots.shape[1]
    rows = lax.broadcasted_iota(jnp.int32, (256, width), 0).astype(f32)

    def picked(first):
        low = (rows == slots[first : first + 1].astype(f32)).astype(bf16)
        high = (rows == slots[first + 1 : first + 2].astype(f32)).astype(bf16)
        return dot(phit_ref[:, :256], low) + dot(phit_ref[:, 256:], high)

    dens = (picked(16) * picked(18)).astype(bf16)
    dens_ref[0] = dens
    fieldt_ref[...] += dot(dens, slots[:16], NT)

    @pl.when(step == pl.num_programs(0) - 1)
    def _():
        split = in_two(fieldt_ref[...].T)
        both = dot(split, pot_ref[...], NT)
        proj_ref[...] = (both[:16] + both[16:]).astype(bf16)


def density(where, phi, slots, eigenpotentials):
    owners, rows, width = slots.shape
    orbs, points = phi.shape
    neig = eigenpotentials.shape[0]
    return pl.pallas_call(
        density_body,
        grid_spec=pltpu.PrefetchScalarGridSpec(
            num_scalar_prefetch=1,
            grid=(owners,),
            in_specs=[
                pl.BlockSpec((orbs, points), lambda i, w: (0, 0)),
                pl.BlockSpec((1, rows, width), lambda i, w: (i, 0, 0)),
                pl.BlockSpec((neig, points), lambda i, w: (0, w[0])),
            ],
            out_specs=[
                pl.BlockSpec((1, points, width), lambda i, w: (i, 0, 0)),
                pl.BlockSpec((16, neig), lambda i, w: (0, 0)),
            ],
            scratch_shapes=[pltpu.VMEM((points, orbs), bf16), pltpu.VMEM((points, 16), f32)],
        ),
        out_shape=[
            jax.ShapeDtypeStruct((owners, points, width), bf16),
            jax.ShapeDtypeStruct((16, neig), bf16),
        ],
        name="density",
    )(where, phi, slots, eigenpotentials)


def direct_body(where_ref, screened_ref, pot_ref, dens_ref, out_ref, field_ref):
    @pl.when(pl.program_id(0) == 0)
    def _():
        half = screened_ref.shape[2]
        total = jnp.zeros(field_ref.shape, f32)
        for core in range(2):
            total += dot(in_two(screened_ref[core]), pot_ref[core * half : (core + 1) * half, :])
        field_ref[...] = total

    split = in_two(field_ref[:16] + field_ref[16:])
    both = dot(split, dens_ref[0])
    out_ref[0] = (both[:16] + both[16:]).astype(bf16)


def direct_terms(where, screened, eigenpotentials, dens):
    owners, points, width = dens.shape
    neig = eigenpotentials.shape[0]
    return pl.pallas_call(
        direct_body,
        grid_spec=pltpu.PrefetchScalarGridSpec(
            num_scalar_prefetch=1,
            grid=(owners,),
            in_specs=[
                pl.BlockSpec(screened.shape, lambda i, w: (0, 0, 0)),
                pl.BlockSpec((neig, points), lambda i, w: (0, w[0])),
                pl.BlockSpec((1, points, width), lambda i, w: (i, 0, 0)),
            ],
            out_specs=pl.BlockSpec((1, 16, width), lambda i, w: (i, 0, 0)),
            scratch_shapes=[pltpu.VMEM((32, points), f32)],
        ),
        out_shape=jax.ShapeDtypeStruct((owners, 16, width), bf16),
        name="direct_terms",
    )(where, screened, eigenpotentials, dens)


def slot_rows(trial_vectors, pair_index):
    low = jnp.where(pair_index < 256, pair_index, -1).astype(bf16)
    high = jnp.where(pair_index >= 256, pair_index - 256, -1).astype(bf16)
    rows = [trial_vectors, low[:1], high[:1], low[1:], high[1:], jnp.zeros((4, trial_vectors.shape[1]), bf16)]
    return jnp.concatenate(rows, axis=0)


def shards(orbitals, eigenpotentials, screening, trial_vectors, pair_index):
    rows, points = orbitals.shape
    part = points // 8
    slots = exchange(copies(slot_rows(trial_vectors, pair_index), 8), GROUP)
    cut = orbitals.reshape(rows, 8, part).transpose(1, 0, 2)
    cut = cut.reshape(2, 1, 2, 2, rows, part)
    sent = jnp.broadcast_to(cut, (2, 4, 2, 2, rows, part)).reshape(32, rows, part)
    phi = exchange(sent, ORB).reshape(32 * rows, part)
    where = lax.axis_index(GROUP).astype(jnp.int32).reshape(1)
    dens, projected = density(where, phi, slots, eigenpotentials)
    neig = projected.shape[1]
    halves = projected.reshape(16, 2, neig // 2).transpose(1, 0, 2)
    halves = copies(halves, 8).reshape(16, 16, neig // 2)
    column = summed(exchange(halves, COLUMN)).astype(bf16)
    half = summed(exchange(copies(column, 16), PLANE))
    scale = lax.dynamic_slice_in_dim(screening, lax.axis_index("c") * (neig // 2), neig // 2, 0)
    screened = lax.all_gather(half * scale[None, :], "c", axis=0)
    terms = direct_terms(where, screened, eigenpotentials, dens)
    owner = summed(exchange(terms, GROUP)).astype(bf16)
    return summed(exchange(copies(owner, 8), SLAB))


def solution(mesh):
    fine = Mesh(mesh.devices.reshape(SIZES), AXES)
    return jax.shard_map(
        shards,
        mesh=fine,
        in_specs=(P(ORB, SLAB), P(None, SLAB), P(), P(None, ORB), P(None, ORB)),
        out_specs=P(None, ORB),
        check_vma=False,
    )
```

```python
import jax
import jax.numpy as jnp
from jax import lax
from jax.experimental import pallas as pl
from jax.experimental.pallas import tpu as pltpu
from jax.sharding import Mesh, PartitionSpec as P

AXES = ("yl", "zh", "zl", "c", "yh", "x")
SIZES = (2, 4, 2, 2, 2, 4)
ORB = ("yl", "zh", "zl", "c")
SLAB = ("yh", "x")
GROUP = ("yl", "zl", "c")
COLUMN = ("zh", "zl", "c")
PLANE = ("yl", "yh", "x")

NB = 16
BLOCK = 128
ROWS = 24
TAKE = 4

f32 = jnp.float32
bf16 = jnp.bfloat16
NT = (((1,), (1,)), ((), ()))
LIMIT = 30 * 1024 * 1024


def exchange(blocks, axes):
    return lax.all_to_all(blocks, axes, 0, 0, tiled=True)


def summed(blocks):
    return jnp.sum(blocks.astype(f32), axis=0)


def copies(value, count):
    return jnp.broadcast_to(value[None], (count, *value.shape))


def in_two(value):
    upper = value.astype(bf16)
    lower = (value - upper.astype(f32)).astype(bf16)
    return jnp.concatenate([upper, lower], axis=0)


def folded(both):
    return both[:NB] + both[NB:]


def dot(left, right, dims=(((1,), (0,)), ((), ()))):
    return lax.dot_general(left, right, dims, preferred_element_type=f32)


def vmem(*values):
    return [pltpu.with_memory_space_constraint(v, pltpu.VMEM) for v in values]


def hbm(*values):
    return [pltpu.with_memory_space_constraint(v, pltpu.HBM) for v in values]


IN_VMEM = pl.BlockSpec(memory_space=pltpu.VMEM)
IN_SMEM = pl.BlockSpec(memory_space=pltpu.SMEM)
IN_HBM = pl.BlockSpec(memory_space=pltpu.HBM)


def prepare_body(orbitals_ref, trial_ref, pair_ref, sent_ref, slots_ref, trials_ref, pairs_ref, sems, in_sems):
    part = sent_ref.shape[2]
    trials = pltpu.make_async_copy(trial_ref, trials_ref, in_sems.at[0])
    pairs = pltpu.make_async_copy(pair_ref, pairs_ref, in_sems.at[1])
    trials.start()
    pairs.start()
    cuts = []
    for group in range(8):
        piece = orbitals_ref.at[:, group * part : (group + 1) * part]
        for layer in range(4):
            to = (group // 4) * 16 + layer * 4 + group % 4
            cuts.append(pltpu.make_async_copy(piece, sent_ref.at[to], sems.at[to]))
    for cut in cuts:
        cut.start()
    pairs.wait()
    index = pairs_ref[...]
    low = jnp.where(index < 256, index, -1)
    high = jnp.where(index >= 256, index - 256, -1)
    where = jnp.concatenate([low, high, low, high], axis=0).astype(f32).astype(bf16)
    trials.wait()
    for block in range(slots_ref.shape[1]):
        lanes = slice(block * BLOCK, (block + 1) * BLOCK)
        for group in range(8):
            slots_ref[group, block, :NB, :] = trials_ref[:, lanes]
            slots_ref[group, block, NB:ROWS, :] = where[:, lanes]
    for cut in cuts:
        cut.wait()


def prepare(orbitals, trial_vectors, pair_index):
    rows, points = orbitals.shape
    blocks = trial_vectors.shape[1] // BLOCK
    return pl.pallas_call(
        prepare_body,
        in_specs=[IN_HBM] * 3,
        out_specs=[IN_VMEM] * 2,
        out_shape=[
            pltpu.VMEM((32, rows, points // 8), bf16),
            pltpu.VMEM((8, blocks, ROWS, BLOCK), bf16),
        ],
        scratch_shapes=[
            pltpu.VMEM(trial_vectors.shape, bf16),
            pltpu.VMEM(pair_index.shape, jnp.int32),
            pltpu.SemaphoreType.DMA((32,)),
            pltpu.SemaphoreType.DMA((2,)),
        ],
        compiler_params=pltpu.CompilerParams(vmem_limit_bytes=LIMIT),
        name="prepare",
    )(*hbm(orbitals, trial_vectors, pair_index))


def density_body(
    group_ref,
    phi_ref,
    slots_ref,
    all_pot_ref,
    kept_ref,
    pot_ref,
    halves_ref,
    list_ref,
    phit_ref,
    fieldt_ref,
    dens_ref,
    sem,
    sems,
):
    points = phit_ref.shape[0]
    fetch = pltpu.make_async_copy(all_pot_ref.at[:, pl.ds(group_ref[0] * points, points)], pot_ref, sem)
    fetch.start()
    phit_ref[...] = phi_ref[...].T
    fieldt_ref[...] = jnp.zeros_like(fieldt_ref)
    blocks = slots_ref.shape[0]
    count = jnp.int32(0)
    for block in range(blocks):
        most = jnp.max(slots_ref[block, NB:ROWS, :].astype(f32))
        list_ref[1 + count] = jnp.int32(block)
        count += (most >= 0.0).astype(jnp.int32)
    list_ref[0] = count
    for extra in range(TAKE):
        list_ref[1 + count + extra] = jnp.int32(0)

    rows = lax.broadcasted_iota(jnp.int32, (256, TAKE * BLOCK), 0).astype(f32)

    def step(turn, unused):
        pieces, trials = [], []
        for k in range(TAKE):
            at = turn * TAKE + k
            block = list_ref[1 + at]
            where = slots_ref[block, NB:ROWS, :].astype(f32)
            pieces.append(jnp.where(at < count, where, -1.0))
            trials.append(slots_ref[block, :NB, :])
        where = jnp.concatenate(pieces, axis=1)
        trial = jnp.concatenate(trials, axis=1)

        def picked(row):
            low = (rows == where[row : row + 1]).astype(bf16)
            high = (rows == where[row + 2 : row + 3]).astype(bf16)
            return dot(phit_ref[...], jnp.concatenate([low, high], axis=0))

        dens = (picked(0) * picked(1)).astype(bf16)
        dens_ref[turn] = dens
        pltpu.make_async_copy(dens_ref.at[turn], kept_ref.at[turn], sems.at[turn]).start()
        fieldt_ref[...] += dot(dens, trial, NT)
        return unused

    turns = (count + TAKE - 1) // TAKE
    lax.fori_loop(0, turns, step, 0)
    fetch.wait()
    proj = folded(dot(in_two(fieldt_ref[...].T), pot_ref[...], NT)).astype(bf16)
    half = halves_ref.shape[2]
    for core in range(2):
        for layer in range(8):
            halves_ref[layer * 2 + core] = proj[:, core * half : (core + 1) * half]

    def kept(turn, unused):
        pltpu.make_async_copy(dens_ref.at[turn], kept_ref.at[turn], sems.at[turn]).wait()
        return unused

    lax.fori_loop(0, turns, kept, 0)


def density(group, phi, slots, eigenpotentials):
    blocks = slots.shape[0]
    orbs, points = phi.shape
    neig = eigenpotentials.shape[0]
    return pl.pallas_call(
        density_body,
        in_specs=[IN_SMEM, IN_VMEM, IN_VMEM, IN_HBM],
        out_specs=[IN_HBM, IN_VMEM, IN_VMEM, IN_SMEM],
        out_shape=[
            pltpu.HBM((blocks // TAKE, points, TAKE * BLOCK), bf16),
            pltpu.VMEM((neig, points), bf16),
            pltpu.VMEM((16, NB, neig // 2), bf16),
            jax.ShapeDtypeStruct((1 + blocks + TAKE,), jnp.int32),
        ],
        scratch_shapes=[
            pltpu.VMEM((points, orbs), bf16),
            pltpu.VMEM((points, NB), f32),
            pltpu.VMEM((blocks // TAKE, points, TAKE * BLOCK), bf16),
            pltpu.SemaphoreType.DMA(()),
            pltpu.SemaphoreType.DMA((blocks // TAKE,)),
        ],
        compiler_params=pltpu.CompilerParams(vmem_limit_bytes=LIMIT),
        name="density",
    )(group, *vmem(phi, slots), *hbm(eigenpotentials))


def direct_body(core_ref, list_ref, mine_ref, other_ref, screening_ref, pot_ref, kept_ref, out_ref, split_ref, dens_ref, sems):
    count = list_ref[0]
    turns = (count + TAKE - 1) // TAKE

    def fetch(turn, unused):
        pltpu.make_async_copy(kept_ref.at[turn], dens_ref.at[turn], sems.at[turn]).start()
        return unused

    lax.fori_loop(0, turns, fetch, 0)
    half = mine_ref.shape[1]
    total = jnp.zeros((NB, pot_ref.shape[1]), f32)
    for ref, core in ((mine_ref, core_ref[0]), (other_ref, 1 - core_ref[0])):
        screened = ref[...] * screening_ref[pl.ds(core, 1), :]
        rows = pot_ref[pl.ds(pl.multiple_of(core * half, half), half), :]
        total += folded(dot(in_two(screened), rows))
    split_ref[...] = in_two(total)
    out_ref[...] = jnp.zeros_like(out_ref)

    def step(turn, unused):
        pltpu.make_async_copy(kept_ref.at[turn], dens_ref.at[turn], sems.at[turn]).wait()
        terms = folded(dot(split_ref[...], dens_ref[turn])).astype(bf16)
        for k in range(TAKE):
            at = turn * TAKE + k

            @pl.when(at < count)
            def _():
                out_ref[list_ref[1 + at]] = terms[:, k * BLOCK : (k + 1) * BLOCK]

        return unused

    lax.fori_loop(0, turns, step, 0)


def direct_terms(core, live, mine, other, screening, pot, dens):
    blocks = dens.shape[0] * TAKE
    return pl.pallas_call(
        direct_body,
        in_specs=[IN_SMEM, IN_SMEM] + [IN_VMEM] * 4 + [IN_HBM],
        out_specs=IN_VMEM,
        out_shape=pltpu.VMEM((blocks, NB, BLOCK), bf16),
        scratch_shapes=[
            pltpu.VMEM((2 * NB, pot.shape[1]), bf16),
            pltpu.VMEM(dens.shape, bf16),
            pltpu.SemaphoreType.DMA((dens.shape[0],)),
        ],
        compiler_params=pltpu.CompilerParams(vmem_limit_bytes=LIMIT),
        name="direct_terms",
    )(core, live, *vmem(mine, other, screening, pot), *hbm(dens))


def shards(orbitals, eigenpotentials, screening, trial_vectors, pair_index):
    neig = eigenpotentials.shape[0]
    group = lax.axis_index(GROUP).astype(jnp.int32).reshape(1)
    core = lax.axis_index("c").astype(jnp.int32).reshape(1)
    scales = screening.reshape(2, neig // 2)
    sent, slots = prepare(orbitals, trial_vectors, pair_index)
    sent, slots, group, core, scales = lax.optimization_barrier((sent, slots, group, core, scales))
    slots = exchange(slots, GROUP)
    slots, sent = lax.optimization_barrier((slots, sent))
    phi = exchange(sent, ORB)
    phi = phi.reshape(32 * phi.shape[1], phi.shape[2])
    slots = slots.reshape(-1, ROWS, BLOCK)
    dens, pot, halves, live = density(group, phi, slots, eigenpotentials)
    column = summed(exchange(halves, COLUMN)).astype(bf16)
    mine = summed(exchange(copies(column, 16), PLANE))
    other = lax.ppermute(mine, "c", [(0, 1), (1, 0)])
    terms = direct_terms(core, live, mine, other, scales, pot, dens)
    terms = exchange(terms.reshape(8, -1, NB, BLOCK), GROUP)
    owner = summed(terms).astype(bf16)
    direct = summed(exchange(copies(owner, 8), SLAB))
    return direct.transpose(1, 0, 2).reshape(NB, -1)


def solution(mesh):
    fine = Mesh(mesh.devices.reshape(SIZES), AXES)
    return jax.shard_map(
        shards,
        mesh=fine,
        in_specs=(P(ORB, SLAB), P(None, SLAB), P(), P(None, ORB), P(None, ORB)),
        out_specs=P(None, ORB),
        check_vma=False,
    )
```

```python
import jax
import jax.numpy as jnp
from jax import lax
from jax.experimental import pallas as pl
from jax.experimental.pallas import tpu as pltpu
from jax.sharding import Mesh, PartitionSpec as P


AXES = ("yl", "zh", "zl", "c", "yh", "x")
SIZES = (2, 4, 2, 2, 2, 4)
ORB = ("yl", "zh", "zl", "c")
SLAB = ("yh", "x")
GROUP = ("yl", "zl")
SOURCES = ("yl", "zh", "zl")
COLUMN = ("zh", "zl", "c")
PLANE = ("yl", "yh", "x")

NB = 16
BLOCK = 128
ROWS = 24
TAKE = 4

f32 = jnp.float32
bf16 = jnp.bfloat16
NT = (((1,), (1,)), ((), ()))
LIMIT = 30 * 1024 * 1024


def exchange(blocks, axes):
    return lax.all_to_all(blocks, axes, 0, 0, tiled=True)


def summed(blocks):
    return jnp.sum(blocks.astype(f32), axis=0)


def copies(value, count):
    return jnp.broadcast_to(value[None], (count, *value.shape))


def in_two(value):
    upper = value.astype(bf16)
    lower = (value - upper.astype(f32)).astype(bf16)
    return jnp.concatenate([upper, lower], axis=0)


def folded(both):
    return both[:NB] + both[NB:]


def dot(left, right, dims=(((1,), (0,)), ((), ()))):
    return lax.dot_general(left, right, dims, preferred_element_type=f32)


def vmem(*values):
    return [pltpu.with_memory_space_constraint(v, pltpu.VMEM) for v in values]


def hbm(*values):
    return [pltpu.with_memory_space_constraint(v, pltpu.HBM) for v in values]


IN_VMEM = pl.BlockSpec(memory_space=pltpu.VMEM)
IN_SMEM = pl.BlockSpec(memory_space=pltpu.SMEM)
IN_HBM = pl.BlockSpec(memory_space=pltpu.HBM)


def prepare_body(orbitals_ref, trial_ref, pair_ref, sent_ref, slots_ref, trials_ref, pairs_ref, sems, in_sems):
    part = sent_ref.shape[2]
    trials = pltpu.make_async_copy(trial_ref, trials_ref, in_sems.at[0])
    pairs = pltpu.make_async_copy(pair_ref, pairs_ref, in_sems.at[1])
    pairs.start()
    trials.start()
    cuts = []
    for to in range(sent_ref.shape[0]):
        group = (to // 8) * 2 + to % 2
        piece = orbitals_ref.at[:, group * part : (group + 1) * part]
        cuts.append(pltpu.make_async_copy(piece, sent_ref.at[to], sems.at[to]))
    for cut in cuts:
        cut.start()
    pairs.wait()
    index = pairs_ref[...]
    place = lax.shift_right_logical(index, 5) * 16 + (index & 15)
    odd = (index & 16) > 0
    even_core = jnp.where((index >= 0) & ~odd, place, -1)
    odd_core = jnp.where((index >= 0) & odd, place, -1)
    where = jnp.concatenate([even_core, odd_core, even_core, odd_core], axis=0).astype(f32).astype(bf16)
    trials.wait()
    for block in range(slots_ref.shape[0]):
        lanes = slice(block * BLOCK, (block + 1) * BLOCK)
        slots_ref[block, :NB, :] = trials_ref[:, lanes]
        slots_ref[block, NB:ROWS, :] = where[:, lanes]
    for cut in cuts:
        cut.wait()


def prepare(orbitals, trial_vectors, pair_index):
    rows, points = orbitals.shape
    blocks = trial_vectors.shape[1] // BLOCK
    return pl.pallas_call(
        prepare_body,
        in_specs=[IN_HBM] * 3,
        out_specs=[IN_VMEM] * 2,
        out_shape=[
            pltpu.VMEM((16, rows, points // 4), bf16),
            pltpu.VMEM((blocks, ROWS, BLOCK), bf16),
        ],
        scratch_shapes=[
            pltpu.VMEM(trial_vectors.shape, bf16),
            pltpu.VMEM(pair_index.shape, jnp.int32),
            pltpu.SemaphoreType.DMA((16,)),
            pltpu.SemaphoreType.DMA((2,)),
        ],
        compiler_params=pltpu.CompilerParams(vmem_limit_bytes=LIMIT),
        name="prepare",
    )(*hbm(orbitals, trial_vectors, pair_index))


def density_body(
    group_ref,
    core_ref,
    mine_ref,
    other_ref,
    slots0_ref,
    slots1_ref,
    slots2_ref,
    slots3_ref,
    all_pot_ref,
    kept_ref,
    pot_ref,
    halves_ref,
    list_ref,
    slots_ref,
    phit_ref,
    fieldt_ref,
    dens_ref,
    sem,
    sems,
):
    points = phit_ref.shape[0]
    group = group_ref[0]
    fetch = pltpu.make_async_copy(all_pot_ref.at[:, pl.ds(group * points, points)], pot_ref, sem)
    fetch.start()
    each = slots0_ref.shape[0]
    for k, ref in enumerate((slots0_ref, slots1_ref, slots2_ref, slots3_ref)):
        slots_ref[pl.ds((group ^ k) * each, each)] = ref[...]
    half = mine_ref.shape[0]
    for core in range(2):

        @pl.when(core_ref[0] == core)
        def _():
            phit_ref[:, core * half : (core + 1) * half] = mine_ref[...].T
            phit_ref[:, (1 - core) * half : (2 - core) * half] = other_ref[...].T

    fieldt_ref[...] = jnp.zeros_like(fieldt_ref)
    blocks = slots_ref.shape[0]
    count = jnp.int32(0)
    for block in range(blocks):
        most = jnp.max(slots_ref[block, NB:ROWS, :].astype(f32))
        list_ref[1 + count] = jnp.int32(block)
        count += (most >= 0.0).astype(jnp.int32)
    list_ref[0] = count
    for extra in range(TAKE):
        list_ref[1 + count + extra] = jnp.int32(0)

    rows = lax.broadcasted_iota(jnp.int32, (half, TAKE * BLOCK), 0).astype(f32)

    def step(turn, unused):
        pieces, trials = [], []
        for k in range(TAKE):
            at = turn * TAKE + k
            block = list_ref[1 + at]
            where = slots_ref[block, NB:ROWS, :].astype(f32)
            pieces.append(jnp.where(at < count, where, -1.0))
            trials.append(slots_ref[block, :NB, :])
        where = jnp.concatenate(pieces, axis=1)
        trial = jnp.concatenate(trials, axis=1)

        def picked(row):
            even_core = (rows == where[row : row + 1]).astype(bf16)
            odd_core = (rows == where[row + 2 : row + 3]).astype(bf16)
            return dot(phit_ref[...], jnp.concatenate([even_core, odd_core], axis=0))

        dens = (picked(0) * picked(1)).astype(bf16)
        dens_ref[turn] = dens
        pltpu.make_async_copy(dens_ref.at[turn], kept_ref.at[turn], sems.at[turn]).start()
        fieldt_ref[...] += dot(dens, trial, NT)
        return unused

    turns = (count + TAKE - 1) // TAKE
    lax.fori_loop(0, turns, step, 0)
    fetch.wait()
    fieldt = fieldt_ref[...]
    upper = fieldt.astype(bf16)
    lower = (fieldt - upper.astype(f32)).astype(bf16)
    projt = dot(pot_ref[...], upper) + dot(pot_ref[...], lower)
    proj = projt.T.astype(bf16)
    width = halves_ref.shape[2]
    for core in range(2):
        for layer in range(8):
            halves_ref[layer * 2 + core] = proj[:, core * width : (core + 1) * width]

    def kept(turn, unused):
        pltpu.make_async_copy(dens_ref.at[turn], kept_ref.at[turn], sems.at[turn]).wait()
        return unused

    lax.fori_loop(0, turns, kept, 0)


def density(group, core, mine, other, slots, eigenpotentials):
    blocks = slots[0].shape[0] * len(slots)
    half, points = mine.shape
    neig = eigenpotentials.shape[0]
    turns = blocks // TAKE
    return pl.pallas_call(
        density_body,
        in_specs=[IN_SMEM] * 2 + [IN_VMEM] * 6 + [IN_HBM],
        out_specs=[IN_HBM, IN_VMEM, IN_VMEM, IN_SMEM],
        out_shape=[
            pltpu.HBM((turns, points, TAKE * BLOCK), bf16),
            pltpu.VMEM((neig, points), bf16),
            pltpu.VMEM((16, NB, neig // 2), bf16),
            jax.ShapeDtypeStruct((1 + blocks + TAKE,), jnp.int32),
        ],
        scratch_shapes=[
            pltpu.VMEM((blocks, ROWS, BLOCK), bf16),
            pltpu.VMEM((points, 2 * half), bf16),
            pltpu.VMEM((points, NB), f32),
            pltpu.VMEM((turns, points, TAKE * BLOCK), bf16),
            pltpu.SemaphoreType.DMA(()),
            pltpu.SemaphoreType.DMA((turns,)),
        ],
        compiler_params=pltpu.CompilerParams(vmem_limit_bytes=LIMIT),
        name="density",
    )(group, core, *vmem(mine, other, *slots), *hbm(eigenpotentials))


def direct_body(core_ref, list_ref, mine_ref, other_ref, screening_ref, pot_ref, kept_ref, out_ref, split_ref, dens_ref, sems):
    count = list_ref[0]
    turns = (count + TAKE - 1) // TAKE

    def fetch(turn, unused):
        pltpu.make_async_copy(kept_ref.at[turn], dens_ref.at[turn], sems.at[turn]).start()
        return unused

    lax.fori_loop(0, turns, fetch, 0)
    half = mine_ref.shape[1]
    total = jnp.zeros((NB, pot_ref.shape[1]), f32)
    for ref, core in ((mine_ref, core_ref[0]), (other_ref, 1 - core_ref[0])):
        scales = jnp.where(core == 0, screening_ref[:, :half], screening_ref[:, half:])
        screened = ref[...] * scales
        rows = pot_ref[pl.ds(pl.multiple_of(core * half, half), half), :]
        total += folded(dot(in_two(screened), rows))
    split_ref[...] = in_two(total)
    out_ref[...] = jnp.zeros_like(out_ref)

    def step(turn, unused):
        pltpu.make_async_copy(kept_ref.at[turn], dens_ref.at[turn], sems.at[turn]).wait()
        terms = folded(dot(split_ref[...], dens_ref[turn])).astype(bf16)
        for k in range(TAKE):
            at = turn * TAKE + k

            @pl.when(at < count)
            def _():
                out_ref[list_ref[1 + at]] = terms[:, k * BLOCK : (k + 1) * BLOCK]

        return unused

    lax.fori_loop(0, turns, step, 0)


def direct_terms(core, live, mine, other, screening, pot, dens):
    blocks = dens.shape[0] * TAKE
    return pl.pallas_call(
        direct_body,
        in_specs=[IN_SMEM, IN_SMEM] + [IN_VMEM] * 4 + [IN_HBM],
        out_specs=IN_VMEM,
        out_shape=pltpu.VMEM((blocks, NB, BLOCK), bf16),
        scratch_shapes=[
            pltpu.VMEM((2 * NB, pot.shape[1]), bf16),
            pltpu.VMEM(dens.shape, bf16),
            pltpu.SemaphoreType.DMA((dens.shape[0],)),
        ],
        compiler_params=pltpu.CompilerParams(vmem_limit_bytes=LIMIT),
        name="direct_terms",
    )(core, live, *vmem(mine, other, screening, pot), *hbm(dens))


def shards(orbitals, eigenpotentials, screening, trial_vectors, pair_index):
    group = lax.axis_index(GROUP).astype(jnp.int32).reshape(1)
    core = lax.axis_index("c").astype(jnp.int32).reshape(1)
    scales = screening.reshape(1, -1)
    sent, own_slots = prepare(orbitals, trial_vectors, pair_index)
    slots = [own_slots]
    for k in range(1, 4):
        slots.append(lax.ppermute(own_slots, GROUP, [(i, i ^ k) for i in range(4)]))
    mine = exchange(sent, SOURCES)
    mine = mine.reshape(-1, mine.shape[2])
    other = lax.ppermute(mine, "c", [(0, 1), (1, 0)])
    dens, pot, halves, live = density(group, core, mine, other, slots, eigenpotentials)
    column = summed(exchange(halves, COLUMN)).astype(bf16)
    part = summed(exchange(copies(column, 16), PLANE))
    apart = lax.ppermute(part, "c", [(0, 1), (1, 0)])
    terms = direct_terms(core, live, part, apart, scales, pot, dens)
    terms = exchange(terms.reshape(4, -1, NB, BLOCK), GROUP)
    owner = summed(terms).astype(bf16)
    direct = summed(exchange(copies(owner, 8), SLAB))
    return direct.transpose(1, 0, 2).reshape(NB, -1)


def solution(mesh):
    fine = Mesh(mesh.devices.reshape(SIZES), AXES)
    return jax.shard_map(
        shards,
        mesh=fine,
        in_specs=(P(ORB, SLAB), P(None, SLAB), P(), P(None, ORB), P(None, ORB)),
        out_specs=P(None, ORB),
        check_vma=False,
    )
```

```python
import jax
import jax.numpy as jnp
from jax import lax
from jax.experimental import pallas as pl
from jax.experimental.pallas import tpu as pltpu
from jax.sharding import Mesh, PartitionSpec as P


AXES = ("yl", "zh", "zl", "c", "yh", "x")
SIZES = (2, 4, 2, 2, 2, 4)
ORB = ("yl", "zh", "zl", "c")
SLAB = ("yh", "x")
GROUP = ("yl", "zl")
SOURCES = ("yl", "zh", "zl")
COLUMN = ("zh", "zl", "c")
WIDE = ("yl", "zl", "yh", "x")

NB = 16
BLOCK = 128
ROWS = 24
TAKE = 4

f32 = jnp.float32
bf16 = jnp.bfloat16
NT = (((1,), (1,)), ((), ()))
LIMIT = 30 * 1024 * 1024


def exchange(blocks, axes):
    return lax.all_to_all(blocks, axes, 0, 0, tiled=True)


def summed(blocks):
    return jnp.sum(blocks.astype(f32), axis=0)


def copies(value, count):
    return jnp.broadcast_to(value[None], (count, *value.shape))


def in_two(value):
    upper = value.astype(bf16)
    lower = (value - upper.astype(f32)).astype(bf16)
    return jnp.concatenate([upper, lower], axis=0)


def folded(both):
    return both[:NB] + both[NB:]


def dot(left, right, dims=(((1,), (0,)), ((), ()))):
    return lax.dot_general(left, right, dims, preferred_element_type=f32)


def vmem(*values):
    return [pltpu.with_memory_space_constraint(v, pltpu.VMEM) for v in values]


def hbm(*values):
    return [pltpu.with_memory_space_constraint(v, pltpu.HBM) for v in values]


IN_VMEM = pl.BlockSpec(memory_space=pltpu.VMEM)
IN_SMEM = pl.BlockSpec(memory_space=pltpu.SMEM)
IN_HBM = pl.BlockSpec(memory_space=pltpu.HBM)


def prepare_body(orbitals_ref, trial_ref, pair_ref, sent_ref, slots_ref, trials_ref, pairs_ref, sems, in_sems):
    part = sent_ref.shape[2]
    trials = pltpu.make_async_copy(trial_ref, trials_ref, in_sems.at[0])
    pairs = pltpu.make_async_copy(pair_ref, pairs_ref, in_sems.at[1])
    pairs.start()
    trials.start()
    cuts = []
    for to in range(sent_ref.shape[0]):
        group = (to // 8) * 2 + to % 2
        piece = orbitals_ref.at[:, group * part : (group + 1) * part]
        cuts.append(pltpu.make_async_copy(piece, sent_ref.at[to], sems.at[to]))
    for cut in cuts:
        cut.start()
    pairs.wait()
    index = pairs_ref[...]
    place = lax.shift_right_logical(index, 5) * 16 + (index & 15)
    odd = (index & 16) > 0
    even_core = jnp.where((index >= 0) & ~odd, place, -1)
    odd_core = jnp.where((index >= 0) & odd, place, -1)
    where = jnp.concatenate([even_core, odd_core, even_core, odd_core], axis=0).astype(f32).astype(bf16)
    trials.wait()
    for block in range(slots_ref.shape[0]):
        lanes = slice(block * BLOCK, (block + 1) * BLOCK)
        slots_ref[block, :NB, :] = trials_ref[:, lanes]
        slots_ref[block, NB:ROWS, :] = where[:, lanes]
    for cut in cuts:
        cut.wait()


def prepare(orbitals, trial_vectors, pair_index):
    rows, points = orbitals.shape
    blocks = trial_vectors.shape[1] // BLOCK
    return pl.pallas_call(
        prepare_body,
        in_specs=[IN_HBM] * 3,
        out_specs=[IN_VMEM] * 2,
        out_shape=[
            pltpu.VMEM((16, rows, points // 4), bf16),
            pltpu.VMEM((blocks, ROWS, BLOCK), bf16),
        ],
        scratch_shapes=[
            pltpu.VMEM(trial_vectors.shape, bf16),
            pltpu.VMEM(pair_index.shape, jnp.int32),
            pltpu.SemaphoreType.DMA((16,)),
            pltpu.SemaphoreType.DMA((2,)),
        ],
        compiler_params=pltpu.CompilerParams(vmem_limit_bytes=LIMIT),
        name="prepare",
    )(*hbm(orbitals, trial_vectors, pair_index))


def density_body(
    group_ref,
    core_ref,
    mine_ref,
    other_ref,
    slots0_ref,
    slots1_ref,
    slots2_ref,
    slots3_ref,
    all_pot_ref,
    kept_ref,
    pot_ref,
    quarters_ref,
    list_ref,
    slots_ref,
    phit_ref,
    fieldt_ref,
    dens_ref,
    sem,
    sems,
):
    points = phit_ref.shape[0]
    group = group_ref[0]
    fetch = pltpu.make_async_copy(all_pot_ref.at[:, pl.ds(group * points, points)], pot_ref, sem)
    fetch.start()
    each = slots0_ref.shape[0]
    for k, ref in enumerate((slots0_ref, slots1_ref, slots2_ref, slots3_ref)):
        slots_ref[pl.ds((group ^ k) * each, each)] = ref[...]
    half = mine_ref.shape[0]
    for core in range(2):

        @pl.when(core_ref[0] == core)
        def _():
            phit_ref[:, core * half : (core + 1) * half] = mine_ref[...].T
            phit_ref[:, (1 - core) * half : (2 - core) * half] = other_ref[...].T

    fieldt_ref[...] = jnp.zeros_like(fieldt_ref)
    blocks = slots_ref.shape[0]
    count = jnp.int32(0)
    for block in range(blocks):
        most = jnp.max(slots_ref[block, NB:ROWS, :].astype(f32))
        list_ref[1 + count] = jnp.int32(block)
        count += (most >= 0.0).astype(jnp.int32)
    list_ref[0] = count
    for extra in range(TAKE):
        list_ref[1 + count + extra] = jnp.int32(0)

    rows = lax.broadcasted_iota(jnp.int32, (half, TAKE * BLOCK), 0).astype(f32)

    def step(turn, unused):
        pieces, trials = [], []
        for k in range(TAKE):
            at = turn * TAKE + k
            block = list_ref[1 + at]
            where = slots_ref[block, NB:ROWS, :].astype(f32)
            pieces.append(jnp.where(at < count, where, -1.0))
            trials.append(slots_ref[block, :NB, :])
        where = jnp.concatenate(pieces, axis=1)
        trial = jnp.concatenate(trials, axis=1)

        def picked(row):
            even_core = (rows == where[row : row + 1]).astype(bf16)
            odd_core = (rows == where[row + 2 : row + 3]).astype(bf16)
            return dot(phit_ref[...], jnp.concatenate([even_core, odd_core], axis=0))

        dens = (picked(0) * picked(1)).astype(bf16)
        dens_ref[turn] = dens
        pltpu.make_async_copy(dens_ref.at[turn], kept_ref.at[turn], sems.at[turn]).start()
        fieldt_ref[...] += dot(dens, trial, NT)
        return unused

    turns = (count + TAKE - 1) // TAKE
    lax.fori_loop(0, turns, step, 0)
    fetch.wait()
    fieldt = fieldt_ref[...]
    upper = fieldt.astype(bf16)
    lower = (fieldt - upper.astype(f32)).astype(bf16)
    projt = dot(pot_ref[...], upper) + dot(pot_ref[...], lower)
    proj = projt.T.astype(bf16)
    width = quarters_ref.shape[2]
    for to in range(16):
        quarter = (to % 2) * 2 + (to // 2) % 2
        quarters_ref[to] = proj[:, quarter * width : (quarter + 1) * width]

    def kept(turn, unused):
        pltpu.make_async_copy(dens_ref.at[turn], kept_ref.at[turn], sems.at[turn]).wait()
        return unused

    lax.fori_loop(0, turns, kept, 0)


def density(group, core, mine, other, slots, eigenpotentials):
    blocks = slots[0].shape[0] * len(slots)
    half, points = mine.shape
    neig = eigenpotentials.shape[0]
    turns = blocks // TAKE
    return pl.pallas_call(
        density_body,
        in_specs=[IN_SMEM] * 2 + [IN_VMEM] * 6 + [IN_HBM],
        out_specs=[IN_HBM, IN_VMEM, IN_VMEM, IN_SMEM],
        out_shape=[
            pltpu.HBM((turns, points, TAKE * BLOCK), bf16),
            pltpu.VMEM((neig, points), bf16),
            pltpu.VMEM((16, NB, neig // 4), bf16),
            jax.ShapeDtypeStruct((1 + blocks + TAKE,), jnp.int32),
        ],
        scratch_shapes=[
            pltpu.VMEM((blocks, ROWS, BLOCK), bf16),
            pltpu.VMEM((points, 2 * half), bf16),
            pltpu.VMEM((points, NB), f32),
            pltpu.VMEM((turns, points, TAKE * BLOCK), bf16),
            pltpu.SemaphoreType.DMA(()),
            pltpu.SemaphoreType.DMA((turns,)),
        ],
        compiler_params=pltpu.CompilerParams(vmem_limit_bytes=LIMIT),
        name="density",
    )(group, core, *vmem(mine, other, *slots), *hbm(eigenpotentials))


def direct_body(core_ref, list_ref, mine_ref, other_ref, screening_ref, pot_ref, kept_ref, out_ref, split_ref, dens_ref, sems):
    count = list_ref[0]
    turns = (count + TAKE - 1) // TAKE

    def fetch(turn, unused):
        pltpu.make_async_copy(kept_ref.at[turn], dens_ref.at[turn], sems.at[turn]).start()
        return unused

    lax.fori_loop(0, turns, fetch, 0)
    half = mine_ref.shape[0] * mine_ref.shape[2]
    total = jnp.zeros((NB, pot_ref.shape[1]), f32)
    for ref, core in ((mine_ref, core_ref[0]), (other_ref, 1 - core_ref[0])):
        scales = jnp.where(core == 0, screening_ref[:, :half], screening_ref[:, half:])
        screened = jnp.concatenate([ref[0], ref[1]], axis=1) * scales
        rows = pot_ref[pl.ds(pl.multiple_of(core * half, half), half), :]
        total += folded(dot(in_two(screened), rows))
    split_ref[...] = in_two(total)
    out_ref[...] = jnp.zeros_like(out_ref)

    def step(turn, unused):
        pltpu.make_async_copy(kept_ref.at[turn], dens_ref.at[turn], sems.at[turn]).wait()
        terms = folded(dot(split_ref[...], dens_ref[turn])).astype(bf16)
        for k in range(TAKE):
            at = turn * TAKE + k

            @pl.when(at < count)
            def _():
                out_ref[list_ref[1 + at]] = terms[:, k * BLOCK : (k + 1) * BLOCK]

        return unused

    lax.fori_loop(0, turns, step, 0)


def direct_terms(core, live, mine, other, screening, pot, dens):
    blocks = dens.shape[0] * TAKE
    return pl.pallas_call(
        direct_body,
        in_specs=[IN_SMEM, IN_SMEM] + [IN_VMEM] * 4 + [IN_HBM],
        out_specs=IN_VMEM,
        out_shape=pltpu.VMEM((blocks, NB, BLOCK), bf16),
        scratch_shapes=[
            pltpu.VMEM((2 * NB, pot.shape[1]), bf16),
            pltpu.VMEM(dens.shape, bf16),
            pltpu.SemaphoreType.DMA((dens.shape[0],)),
        ],
        compiler_params=pltpu.CompilerParams(vmem_limit_bytes=LIMIT),
        name="direct_terms",
    )(core, live, *vmem(mine, other, screening, pot), *hbm(dens))


def shards(orbitals, eigenpotentials, screening, trial_vectors, pair_index):
    group = lax.axis_index(GROUP).astype(jnp.int32).reshape(1)
    core = lax.axis_index("c").astype(jnp.int32).reshape(1)
    scales = screening.reshape(1, -1)
    sent, own_slots = prepare(orbitals, trial_vectors, pair_index)
    slots = [own_slots]
    for k in range(1, 4):
        slots.append(lax.ppermute(own_slots, GROUP, [(i, i ^ k) for i in range(4)]))
    mine = exchange(sent, SOURCES)
    mine = mine.reshape(-1, mine.shape[2])
    other = lax.ppermute(mine, "c", [(0, 1), (1, 0)])
    dens, pot, quarters, live = density(group, core, mine, other, slots, eigenpotentials)
    column = summed(exchange(quarters, COLUMN)).astype(bf16)
    wide = exchange(copies(column, 32), WIDE)
    part = jnp.sum(wide.reshape(2, 2, 8, *column.shape).astype(f32), axis=(0, 2))
    apart = lax.ppermute(part, "c", [(0, 1), (1, 0)])
    terms = direct_terms(core, live, part, apart, scales, pot, dens)
    terms = exchange(terms.reshape(4, -1, NB, BLOCK), GROUP)
    owner = summed(terms).astype(bf16)
    direct = summed(exchange(copies(owner, 8), SLAB))
    return direct.transpose(1, 0, 2).reshape(NB, -1)


def solution(mesh):
    fine = Mesh(mesh.devices.reshape(SIZES), AXES)
    return jax.shard_map(
        shards,
        mesh=fine,
        in_specs=(P(ORB, SLAB), P(None, SLAB), P(), P(None, ORB), P(None, ORB)),
        out_specs=P(None, ORB),
        check_vma=False,
    )
```

```python
import jax
import jax.numpy as jnp
from jax import lax
from jax.experimental import pallas as pl
from jax.experimental.pallas import tpu as pltpu
from jax.sharding import Mesh, PartitionSpec as P


AXES = ("yl", "zh", "zl", "c", "yh", "x")
SIZES = (2, 4, 2, 2, 2, 4)
ORB = ("yl", "zh", "zl", "c")
SLAB = ("yh", "x")
GROUP = ("yl", "zl")
SOURCES = ("yl", "zh", "zl")
COLUMN = ("zh", "zl", "c")
WIDE = ("yl", "zl", "yh", "x")

NB = 16
BLOCK = 128
ROWS = 24
TAKE = 4

f32 = jnp.float32
bf16 = jnp.bfloat16
NT = (((1,), (1,)), ((), ()))
LIMIT = 30 * 1024 * 1024


def exchange(blocks, axes):
    return lax.all_to_all(blocks, axes, 0, 0, tiled=True)


def summed(blocks):
    return jnp.sum(blocks.astype(f32), axis=0)


def copies(value, count):
    return jnp.broadcast_to(value[None], (count, *value.shape))


def in_two(value):
    upper = value.astype(bf16)
    lower = (value - upper.astype(f32)).astype(bf16)
    return jnp.concatenate([upper, lower], axis=0)


def folded(both):
    return both[:NB] + both[NB:]


def dot(left, right, dims=(((1,), (0,)), ((), ()))):
    return lax.dot_general(left, right, dims, preferred_element_type=f32)


def vmem(*values):
    return [pltpu.with_memory_space_constraint(v, pltpu.VMEM) for v in values]


def hbm(*values):
    return [pltpu.with_memory_space_constraint(v, pltpu.HBM) for v in values]


IN_VMEM = pl.BlockSpec(memory_space=pltpu.VMEM)
IN_SMEM = pl.BlockSpec(memory_space=pltpu.SMEM)
IN_HBM = pl.BlockSpec(memory_space=pltpu.HBM)


def prepare_body(orbitals_ref, trial_ref, pair_ref, sent_ref, slots_ref, trials_ref, pairs_ref, sems, in_sems):
    part = sent_ref.shape[2]
    trials = pltpu.make_async_copy(trial_ref, trials_ref, in_sems.at[0])
    pairs = pltpu.make_async_copy(pair_ref, pairs_ref, in_sems.at[1])
    pairs.start()
    trials.start()
    cuts = []
    for to in range(sent_ref.shape[0]):
        group = (to // 8) * 2 + to % 2
        piece = orbitals_ref.at[:, group * part : (group + 1) * part]
        cuts.append(pltpu.make_async_copy(piece, sent_ref.at[to], sems.at[to]))
    for cut in cuts:
        cut.start()
    pairs.wait()
    index = pairs_ref[...]
    place = lax.shift_right_logical(index, 5) * 16 + (index & 15)
    odd = (index & 16) > 0
    even_core = jnp.where((index >= 0) & ~odd, place, -1)
    odd_core = jnp.where((index >= 0) & odd, place, -1)
    where = jnp.concatenate([even_core, odd_core, even_core, odd_core], axis=0).astype(f32).astype(bf16)
    trials.wait()
    for block in range(slots_ref.shape[0]):
        lanes = slice(block * BLOCK, (block + 1) * BLOCK)
        slots_ref[block, :NB, :] = trials_ref[:, lanes]
        slots_ref[block, NB:ROWS, :] = where[:, lanes]
    for cut in cuts:
        cut.wait()


def prepare(orbitals, trial_vectors, pair_index):
    rows, points = orbitals.shape
    blocks = trial_vectors.shape[1] // BLOCK
    return pl.pallas_call(
        prepare_body,
        in_specs=[IN_HBM] * 3,
        out_specs=[IN_VMEM] * 2,
        out_shape=[
            pltpu.VMEM((16, rows, points // 4), bf16),
            pltpu.VMEM((blocks, ROWS, BLOCK), bf16),
        ],
        scratch_shapes=[
            pltpu.VMEM(trial_vectors.shape, bf16),
            pltpu.VMEM(pair_index.shape, jnp.int32),
            pltpu.SemaphoreType.DMA((16,)),
            pltpu.SemaphoreType.DMA((2,)),
        ],
        compiler_params=pltpu.CompilerParams(vmem_limit_bytes=LIMIT),
        name="prepare",
    )(*hbm(orbitals, trial_vectors, pair_index))


def density_body(
    group_ref,
    core_ref,
    mine_ref,
    other_ref,
    slots0_ref,
    slots1_ref,
    slots2_ref,
    slots3_ref,
    all_pot_ref,
    kept_ref,
    pot_ref,
    quarters_ref,
    list_ref,
    slots_ref,
    phit_ref,
    fieldt_ref,
    dens_ref,
    sem,
    sems,
):
    points = phit_ref.shape[0]
    group = group_ref[0]
    fetch = pltpu.make_async_copy(all_pot_ref.at[:, pl.ds(group * points, points)], pot_ref, sem)
    fetch.start()
    each = slots0_ref.shape[0]
    for k, ref in enumerate((slots0_ref, slots1_ref, slots2_ref, slots3_ref)):
        slots_ref[pl.ds((group ^ k) * each, each)] = ref[...]
    half = mine_ref.shape[0]
    for core in range(2):

        @pl.when(core_ref[0] == core)
        def _():
            phit_ref[:, core * half : (core + 1) * half] = mine_ref[...].T
            phit_ref[:, (1 - core) * half : (2 - core) * half] = other_ref[...].T

    fieldt_ref[...] = jnp.zeros_like(fieldt_ref)
    blocks = slots_ref.shape[0]
    count = jnp.int32(0)
    for block in range(blocks):
        most = jnp.max(slots_ref[block, NB:ROWS, :].astype(f32))
        list_ref[1 + count] = jnp.int32(block)
        count += (most >= 0.0).astype(jnp.int32)
    list_ref[0] = count
    for extra in range(TAKE):
        list_ref[1 + count + extra] = jnp.int32(0)

    rows = lax.broadcasted_iota(jnp.int32, (half, TAKE * BLOCK), 0).astype(f32)

    def step(turn, unused):
        pieces, trials = [], []
        for k in range(TAKE):
            at = turn * TAKE + k
            block = list_ref[1 + at]
            where = slots_ref[block, NB:ROWS, :].astype(f32)
            pieces.append(jnp.where(at < count, where, -1.0))
            trials.append(slots_ref[block, :NB, :])
        where = jnp.concatenate(pieces, axis=1)
        trial = jnp.concatenate(trials, axis=1)

        def picked(row):
            even_core = (rows == where[row : row + 1]).astype(bf16)
            odd_core = (rows == where[row + 2 : row + 3]).astype(bf16)
            return dot(phit_ref[...], jnp.concatenate([even_core, odd_core], axis=0))

        dens = (picked(0) * picked(1)).astype(bf16)
        dens_ref[turn] = dens
        pltpu.make_async_copy(dens_ref.at[turn], kept_ref.at[turn], sems.at[turn]).start()
        fieldt_ref[...] += dot(dens, trial, NT)
        return unused

    turns = (count + TAKE - 1) // TAKE
    lax.fori_loop(0, turns, step, 0)
    fetch.wait()
    fieldt = fieldt_ref[...]
    upper = fieldt.astype(bf16)
    lower = (fieldt - upper.astype(f32)).astype(bf16)
    proj = folded(dot(pot_ref[...], jnp.concatenate([upper, lower], axis=1)).T).astype(bf16)
    width = quarters_ref.shape[2]
    for to in range(16):
        quarter = (to % 2) * 2 + (to // 2) % 2
        quarters_ref[to] = proj[:, quarter * width : (quarter + 1) * width]

    def kept(turn, unused):
        pltpu.make_async_copy(dens_ref.at[turn], kept_ref.at[turn], sems.at[turn]).wait()
        return unused

    lax.fori_loop(0, turns, kept, 0)


def density(group, core, mine, other, slots, eigenpotentials):
    blocks = slots[0].shape[0] * len(slots)
    half, points = mine.shape
    neig = eigenpotentials.shape[0]
    turns = blocks // TAKE
    return pl.pallas_call(
        density_body,
        in_specs=[IN_SMEM] * 2 + [IN_VMEM] * 6 + [IN_HBM],
        out_specs=[IN_HBM, IN_VMEM, IN_VMEM, IN_SMEM],
        out_shape=[
            pltpu.HBM((turns, points, TAKE * BLOCK), bf16),
            pltpu.VMEM((neig, points), bf16),
            pltpu.VMEM((16, NB, neig // 4), bf16),
            jax.ShapeDtypeStruct((1 + blocks + TAKE,), jnp.int32),
        ],
        scratch_shapes=[
            pltpu.VMEM((blocks, ROWS, BLOCK), bf16),
            pltpu.VMEM((points, 2 * half), bf16),
            pltpu.VMEM((points, NB), f32),
            pltpu.VMEM((turns, points, TAKE * BLOCK), bf16),
            pltpu.SemaphoreType.DMA(()),
            pltpu.SemaphoreType.DMA((turns,)),
        ],
        compiler_params=pltpu.CompilerParams(vmem_limit_bytes=LIMIT),
        name="density",
    )(group, core, *vmem(mine, other, *slots), *hbm(eigenpotentials))


def direct_body(
    group_ref,
    core_ref,
    list_ref,
    mine_ref,
    other_ref,
    screening_ref,
    pot_ref,
    kept_ref,
    out0_ref,
    out1_ref,
    out2_ref,
    out3_ref,
    terms_ref,
    split_ref,
    dens_ref,
    sems,
):
    count = list_ref[0]
    turns = (count + TAKE - 1) // TAKE

    def fetch(turn, unused):
        pltpu.make_async_copy(kept_ref.at[turn], dens_ref.at[turn], sems.at[turn]).start()
        return unused

    lax.fori_loop(0, turns, fetch, 0)
    terms_ref[...] = jnp.zeros_like(terms_ref)
    half = mine_ref.shape[0] * mine_ref.shape[2]
    total = jnp.zeros((NB, pot_ref.shape[1]), f32)
    for ref, core in ((mine_ref, core_ref[0]), (other_ref, 1 - core_ref[0])):
        scales = jnp.where(core == 0, screening_ref[:, :half], screening_ref[:, half:])
        screened = jnp.concatenate([ref[0], ref[1]], axis=1) * scales
        rows = pot_ref[pl.ds(pl.multiple_of(core * half, half), half), :]
        total += folded(dot(in_two(screened), rows))
    split_ref[...] = in_two(total)
    each = out0_ref.shape[0]
    own = group_ref[0] * each

    def step(turn, unused):
        pltpu.make_async_copy(kept_ref.at[turn], dens_ref.at[turn], sems.at[turn]).wait()
        terms = folded(dot(split_ref[...], dens_ref[turn])).astype(bf16)
        for k in range(TAKE):
            at = turn * TAKE + k

            @pl.when(at < count)
            def _():
                terms_ref[list_ref[1 + at] ^ own] = terms[:, k * BLOCK : (k + 1) * BLOCK]

        return unused

    lax.fori_loop(0, turns, step, 0)
    for k, ref in enumerate((out0_ref, out1_ref, out2_ref, out3_ref)):
        ref[...] = terms_ref[k * each : (k + 1) * each]


def direct_terms(group, core, live, mine, other, screening, pot, dens):
    blocks = dens.shape[0] * TAKE
    return pl.pallas_call(
        direct_body,
        in_specs=[IN_SMEM] * 3 + [IN_VMEM] * 4 + [IN_HBM],
        out_specs=[IN_VMEM] * 4,
        out_shape=[pltpu.VMEM((blocks // 4, NB, BLOCK), bf16)] * 4,
        scratch_shapes=[
            pltpu.VMEM((blocks, NB, BLOCK), bf16),
            pltpu.VMEM((2 * NB, pot.shape[1]), bf16),
            pltpu.VMEM(dens.shape, bf16),
            pltpu.SemaphoreType.DMA((dens.shape[0],)),
        ],
        compiler_params=pltpu.CompilerParams(vmem_limit_bytes=LIMIT),
        name="direct_terms",
    )(group, core, live, *vmem(mine, other, screening, pot), *hbm(dens))


def shards(orbitals, eigenpotentials, screening, trial_vectors, pair_index):
    group = lax.axis_index(GROUP).astype(jnp.int32).reshape(1)
    core = lax.axis_index("c").astype(jnp.int32).reshape(1)
    scales = screening.reshape(1, -1)
    sent, own_slots = prepare(orbitals, trial_vectors, pair_index)
    slots = [own_slots]
    for k in range(1, 4):
        slots.append(lax.ppermute(own_slots, GROUP, [(i, i ^ k) for i in range(4)]))
    mine = exchange(sent, SOURCES)
    mine = mine.reshape(-1, mine.shape[2])
    other = lax.ppermute(mine, "c", [(0, 1), (1, 0)])
    dens, pot, quarters, live = density(group, core, mine, other, slots, eigenpotentials)
    column = summed(exchange(quarters, COLUMN)).astype(bf16)
    wide = exchange(copies(column, 32), WIDE)
    part = jnp.sum(wide.reshape(2, 2, 8, *column.shape).astype(f32), axis=(0, 2))
    apart = lax.ppermute(part, "c", [(0, 1), (1, 0)])
    terms = direct_terms(group, core, live, part, apart, scales, pot, dens)
    owner = terms[0].astype(f32)
    for k in range(1, 4):
        owner += lax.ppermute(terms[k], GROUP, [(i, i ^ k) for i in range(4)]).astype(f32)
    owner = owner.astype(bf16)
    direct = summed(exchange(copies(owner, 8), SLAB))
    return direct.transpose(1, 0, 2).reshape(NB, -1)


def solution(mesh):
    fine = Mesh(mesh.devices.reshape(SIZES), AXES)
    return jax.shard_map(
        shards,
        mesh=fine,
        in_specs=(P(ORB, SLAB), P(None, SLAB), P(), P(None, ORB), P(None, ORB)),
        out_specs=P(None, ORB),
        check_vma=False,
    )
```

```python
import jax
import jax.numpy as jnp
from jax import lax
from jax.experimental import pallas as pl
from jax.experimental.pallas import tpu as pltpu
from jax.sharding import Mesh, PartitionSpec as P


AXES = ("yl", "zh", "zl", "c", "yh", "x")
SIZES = (2, 4, 2, 2, 2, 4)
ORB = ("yl", "zh", "zl", "c")
SLAB = ("yh", "x")
GROUP = ("yl", "zl")
SOURCES = ("yl", "zh", "zl")
FAR = ("zh", "yh", "x")

NB = 16
BLOCK = 128
EIGHTH = 128
ROWS = 24
TAKE = 4

f32 = jnp.float32
bf16 = jnp.bfloat16
NT = (((1,), (1,)), ((), ()))
LIMIT = 30 * 1024 * 1024


def exchange(blocks, axes):
    return lax.all_to_all(blocks, axes, 0, 0, tiled=True)


def swapped(value):
    return lax.ppermute(value, "c", [(0, 1), (1, 0)])


def passed(value, k):
    return lax.ppermute(value, GROUP, [(i, i ^ k) for i in range(4)])


def summed(blocks):
    return jnp.sum(blocks.astype(f32), axis=0)


def copies(value, count):
    return jnp.broadcast_to(value[None], (count, *value.shape))


def in_two(value):
    upper = value.astype(bf16)
    lower = (value - upper.astype(f32)).astype(bf16)
    return jnp.concatenate([upper, lower], axis=0)


def folded(both):
    return both[:NB] + both[NB:]


def dot(left, right, dims=(((1,), (0,)), ((), ()))):
    return lax.dot_general(left, right, dims, preferred_element_type=f32)


def vmem(*values):
    return [pltpu.with_memory_space_constraint(v, pltpu.VMEM) for v in values]


def hbm(*values):
    return [pltpu.with_memory_space_constraint(v, pltpu.HBM) for v in values]


IN_VMEM = pl.BlockSpec(memory_space=pltpu.VMEM)
IN_SMEM = pl.BlockSpec(memory_space=pltpu.SMEM)
IN_HBM = pl.BlockSpec(memory_space=pltpu.HBM)


def prepare_body(orbitals_ref, trial_ref, pair_ref, sent_ref, slots_ref, trials_ref, pairs_ref, sems, in_sems):
    part = sent_ref.shape[2]
    trials = pltpu.make_async_copy(trial_ref, trials_ref, in_sems.at[0])
    pairs = pltpu.make_async_copy(pair_ref, pairs_ref, in_sems.at[1])
    pairs.start()
    trials.start()
    cuts = []
    for to in range(sent_ref.shape[0]):
        group = (to // 8) * 2 + to % 2
        piece = orbitals_ref.at[:, group * part : (group + 1) * part]
        cuts.append(pltpu.make_async_copy(piece, sent_ref.at[to], sems.at[to]))
    for cut in cuts:
        cut.start()
    pairs.wait()
    index = pairs_ref[...]
    place = lax.shift_right_logical(index, 5) * 16 + (index & 15)
    odd = (index & 16) > 0
    even_core = jnp.where((index >= 0) & ~odd, place, -1)
    odd_core = jnp.where((index >= 0) & odd, place, -1)
    where = jnp.concatenate([even_core, odd_core, even_core, odd_core], axis=0).astype(f32).astype(bf16)
    trials.wait()
    for block in range(slots_ref.shape[0]):
        lanes = slice(block * BLOCK, (block + 1) * BLOCK)
        slots_ref[block, :NB, :] = trials_ref[:, lanes]
        slots_ref[block, NB:ROWS, :] = where[:, lanes]
    for cut in cuts:
        cut.wait()


def prepare(orbitals, trial_vectors, pair_index):
    rows, points = orbitals.shape
    blocks = trial_vectors.shape[1] // BLOCK
    return pl.pallas_call(
        prepare_body,
        in_specs=[IN_HBM] * 3,
        out_specs=[IN_VMEM] * 2,
        out_shape=[
            pltpu.VMEM((16, rows, points // 4), bf16),
            pltpu.VMEM((blocks, ROWS, BLOCK), bf16),
        ],
        scratch_shapes=[
            pltpu.VMEM(trial_vectors.shape, bf16),
            pltpu.VMEM(pair_index.shape, jnp.int32),
            pltpu.SemaphoreType.DMA((16,)),
            pltpu.SemaphoreType.DMA((2,)),
        ],
        compiler_params=pltpu.CompilerParams(vmem_limit_bytes=LIMIT),
        name="prepare",
    )(*hbm(orbitals, trial_vectors, pair_index))


def density_body(
    group_ref,
    core_ref,
    mine_ref,
    other_ref,
    slots0_ref,
    slots1_ref,
    slots2_ref,
    slots3_ref,
    all_pot_ref,
    kept_ref,
    pot_ref,
    keep_ref,
    give_ref,
    list_ref,
    slots_ref,
    phit_ref,
    fieldt_ref,
    pieces_ref,
    dens_ref,
    sem,
    sems,
):
    points = phit_ref.shape[0]
    group = group_ref[0]
    fetch = pltpu.make_async_copy(all_pot_ref.at[:, pl.ds(group * points, points)], pot_ref, sem)
    fetch.start()
    each = slots0_ref.shape[0]
    for k, ref in enumerate((slots0_ref, slots1_ref, slots2_ref, slots3_ref)):
        slots_ref[pl.ds((group ^ k) * each, each)] = ref[...]
    half = mine_ref.shape[0]
    for core in range(2):

        @pl.when(core_ref[0] == core)
        def _():
            phit_ref[:, core * half : (core + 1) * half] = mine_ref[...].T
            phit_ref[:, (1 - core) * half : (2 - core) * half] = other_ref[...].T

    fieldt_ref[...] = jnp.zeros_like(fieldt_ref)
    blocks = slots_ref.shape[0]
    count = jnp.int32(0)
    for block in range(blocks):
        most = jnp.max(slots_ref[block, NB:ROWS, :].astype(f32))
        list_ref[1 + count] = jnp.int32(block)
        count += (most >= 0.0).astype(jnp.int32)
    list_ref[0] = count
    for extra in range(TAKE):
        list_ref[1 + count + extra] = jnp.int32(0)

    rows = lax.broadcasted_iota(jnp.int32, (half, TAKE * BLOCK), 0).astype(f32)

    def step(turn, unused):
        pieces, trials = [], []
        for k in range(TAKE):
            at = turn * TAKE + k
            block = list_ref[1 + at]
            where = slots_ref[block, NB:ROWS, :].astype(f32)
            pieces.append(jnp.where(at < count, where, -1.0))
            trials.append(slots_ref[block, :NB, :])
        where = jnp.concatenate(pieces, axis=1)
        trial = jnp.concatenate(trials, axis=1)

        def picked(row):
            even_core = (rows == where[row : row + 1]).astype(bf16)
            odd_core = (rows == where[row + 2 : row + 3]).astype(bf16)
            return dot(phit_ref[...], jnp.concatenate([even_core, odd_core], axis=0))

        dens = (picked(0) * picked(1)).astype(bf16)
        dens_ref[turn] = dens
        pltpu.make_async_copy(dens_ref.at[turn], kept_ref.at[turn], sems.at[turn]).start()
        fieldt_ref[...] += dot(dens, trial, NT)
        return unused

    turns = (count + TAKE - 1) // TAKE
    lax.fori_loop(0, turns, step, 0)
    fetch.wait()
    fieldt = fieldt_ref[...]
    upper = fieldt.astype(bf16)
    lower = (fieldt - upper.astype(f32)).astype(bf16)
    proj = folded(dot(pot_ref[...], jnp.concatenate([upper, lower], axis=1)).T).astype(bf16)
    for piece in range(8):
        pieces_ref[piece] = proj[:, piece * EIGHTH : (piece + 1) * EIGHTH]
    core = core_ref[0]
    for k in range(4):
        keep_ref[k] = pieces_ref[core * 4 + (group ^ k)]
        give_ref[k] = pieces_ref[(1 - core) * 4 + (group ^ k)]

    def kept(turn, unused):
        pltpu.make_async_copy(dens_ref.at[turn], kept_ref.at[turn], sems.at[turn]).wait()
        return unused

    lax.fori_loop(0, turns, kept, 0)


def density(group, core, mine, other, slots, eigenpotentials):
    blocks = slots[0].shape[0] * len(slots)
    half, points = mine.shape
    neig = eigenpotentials.shape[0]
    turns = blocks // TAKE
    return pl.pallas_call(
        density_body,
        in_specs=[IN_SMEM] * 2 + [IN_VMEM] * 6 + [IN_HBM],
        out_specs=[IN_HBM, IN_VMEM, IN_VMEM, IN_VMEM, IN_SMEM],
        out_shape=[
            pltpu.HBM((turns, points, TAKE * BLOCK), bf16),
            pltpu.VMEM((neig, points), bf16),
            pltpu.VMEM((4, NB, EIGHTH), bf16),
            pltpu.VMEM((4, NB, EIGHTH), bf16),
            jax.ShapeDtypeStruct((1 + blocks + TAKE,), jnp.int32),
        ],
        scratch_shapes=[
            pltpu.VMEM((blocks, ROWS, BLOCK), bf16),
            pltpu.VMEM((points, 2 * half), bf16),
            pltpu.VMEM((points, NB), f32),
            pltpu.VMEM((8, NB, EIGHTH), bf16),
            pltpu.VMEM((turns, points, TAKE * BLOCK), bf16),
            pltpu.SemaphoreType.DMA(()),
            pltpu.SemaphoreType.DMA((turns,)),
        ],
        compiler_params=pltpu.CompilerParams(vmem_limit_bytes=LIMIT),
        name="density",
    )(group, core, *vmem(mine, other, *slots), *hbm(eigenpotentials))


def direct_body(
    group_ref,
    core_ref,
    list_ref,
    both0_ref,
    both1_ref,
    both2_ref,
    both3_ref,
    screening_ref,
    pot_ref,
    kept_ref,
    out0_ref,
    out1_ref,
    out2_ref,
    out3_ref,
    pieces_ref,
    terms_ref,
    split_ref,
    dens_ref,
    sems,
):
    count = list_ref[0]
    turns = (count + TAKE - 1) // TAKE

    def fetch(turn, unused):
        pltpu.make_async_copy(kept_ref.at[turn], dens_ref.at[turn], sems.at[turn]).start()
        return unused

    lax.fori_loop(0, turns, fetch, 0)
    terms_ref[...] = jnp.zeros_like(terms_ref)
    core = core_ref[0]
    for k, ref in enumerate((both0_ref, both1_ref, both2_ref, both3_ref)):
        pieces_ref[core * 4 + (group_ref[0] ^ k)] = ref[0]
        pieces_ref[(1 - core) * 4 + (group_ref[0] ^ k)] = ref[1]
    projected = jnp.concatenate([pieces_ref[piece] for piece in range(8)], axis=1)
    screened = projected * screening_ref[...]
    split_ref[...] = in_two(folded(dot(in_two(screened), pot_ref[...])))
    each = out0_ref.shape[0]
    own = group_ref[0] * each

    def step(turn, unused):
        pltpu.make_async_copy(kept_ref.at[turn], dens_ref.at[turn], sems.at[turn]).wait()
        terms = folded(dot(split_ref[...], dens_ref[turn])).astype(bf16)
        for k in range(TAKE):
            at = turn * TAKE + k

            @pl.when(at < count)
            def _():
                terms_ref[list_ref[1 + at] ^ own] = terms[:, k * BLOCK : (k + 1) * BLOCK]

        return unused

    lax.fori_loop(0, turns, step, 0)
    for k, ref in enumerate((out0_ref, out1_ref, out2_ref, out3_ref)):
        ref[...] = terms_ref[k * each : (k + 1) * each]


def direct_terms(group, core, live, both, screening, pot, dens):
    blocks = dens.shape[0] * TAKE
    return pl.pallas_call(
        direct_body,
        in_specs=[IN_SMEM] * 3 + [IN_VMEM] * 6 + [IN_HBM],
        out_specs=[IN_VMEM] * 4,
        out_shape=[pltpu.VMEM((blocks // 4, NB, BLOCK), bf16)] * 4,
        scratch_shapes=[
            pltpu.VMEM((8, NB, EIGHTH), f32),
            pltpu.VMEM((blocks, NB, BLOCK), bf16),
            pltpu.VMEM((2 * NB, pot.shape[1]), bf16),
            pltpu.VMEM(dens.shape, bf16),
            pltpu.SemaphoreType.DMA((dens.shape[0],)),
        ],
        compiler_params=pltpu.CompilerParams(vmem_limit_bytes=LIMIT),
        name="direct_terms",
    )(group, core, live, *vmem(*both, screening, pot), *hbm(dens))


def shards(orbitals, eigenpotentials, screening, trial_vectors, pair_index):
    group = lax.axis_index(GROUP).astype(jnp.int32).reshape(1)
    core = lax.axis_index("c").astype(jnp.int32).reshape(1)
    scales = screening.reshape(1, -1)
    sent, own_slots = prepare(orbitals, trial_vectors, pair_index)
    slots = [own_slots]
    for k in range(1, 4):
        slots.append(passed(own_slots, k))
    mine = exchange(sent, SOURCES)
    mine = mine.reshape(-1, mine.shape[2])
    other = swapped(mine)
    dens, pot, keep, give, live = density(group, core, mine, other, slots, eigenpotentials)
    half = (keep.astype(f32) + swapped(give).astype(f32)).astype(bf16)
    eighth = half[0].astype(f32)
    for k in range(1, 4):
        eighth += passed(half[k], k).astype(f32)
    whole = summed(exchange(copies(eighth.astype(bf16), 32), FAR))
    pair = jnp.stack([whole, swapped(whole)])
    both = [pair] + [passed(pair, k) for k in range(1, 4)]
    terms = direct_terms(group, core, live, both, scales, pot, dens)
    owner = terms[0].astype(f32)
    for k in range(1, 4):
        owner += passed(terms[k], k).astype(f32)
    owner = owner.astype(bf16)
    direct = summed(exchange(copies(owner, 8), SLAB))
    return direct.transpose(1, 0, 2).reshape(NB, -1)


def solution(mesh):
    fine = Mesh(mesh.devices.reshape(SIZES), AXES)
    return jax.shard_map(
        shards,
        mesh=fine,
        in_specs=(P(ORB, SLAB), P(None, SLAB), P(), P(None, ORB), P(None, ORB)),
        out_specs=P(None, ORB),
        check_vma=False,
    )
```

```python
import jax
import jax.numpy as jnp
from jax import lax
from jax.experimental import pallas as pl
from jax.experimental.pallas import tpu as pltpu
from jax.sharding import Mesh, PartitionSpec as P


AXES = ("yl", "zh", "zl", "c", "yh", "x")
SIZES = (2, 4, 2, 2, 2, 4)
ORB = ("yl", "zh", "zl", "c")
SLAB = ("yh", "x")
GROUP = ("yl", "zl")
SOURCES = ("yl", "zh", "zl")
COLUMN = ("zh", "zl")
WIDE = ("yl", "zl", "yh", "x")

NB = 16
BLOCK = 128
ROWS = 24
TAKE = 4

f32 = jnp.float32
bf16 = jnp.bfloat16
NT = (((1,), (1,)), ((), ()))
LIMIT = 30 * 1024 * 1024


def exchange(blocks, axes):
    return lax.all_to_all(blocks, axes, 0, 0, tiled=True)


def summed(blocks):
    return jnp.sum(blocks.astype(f32), axis=0)


def copies(value, count):
    return jnp.broadcast_to(value[None], (count, *value.shape))


def in_two(value):
    upper = value.astype(bf16)
    lower = (value - upper.astype(f32)).astype(bf16)
    return jnp.concatenate([upper, lower], axis=0)


def folded(both):
    return both[:NB] + both[NB:]


def dot(left, right, dims=(((1,), (0,)), ((), ()))):
    return lax.dot_general(left, right, dims, preferred_element_type=f32)


def vmem(*values):
    return [pltpu.with_memory_space_constraint(v, pltpu.VMEM) for v in values]


def hbm(*values):
    return [pltpu.with_memory_space_constraint(v, pltpu.HBM) for v in values]


IN_VMEM = pl.BlockSpec(memory_space=pltpu.VMEM)
IN_SMEM = pl.BlockSpec(memory_space=pltpu.SMEM)
IN_HBM = pl.BlockSpec(memory_space=pltpu.HBM)


def prepare_body(orbitals_ref, trial_ref, pair_ref, sent_ref, slots_ref, trials_ref, pairs_ref, sems, in_sems):
    part = sent_ref.shape[2]
    trials = pltpu.make_async_copy(trial_ref, trials_ref, in_sems.at[0])
    pairs = pltpu.make_async_copy(pair_ref, pairs_ref, in_sems.at[1])
    pairs.start()
    trials.start()
    cuts = []
    for to in range(sent_ref.shape[0]):
        group = (to // 8) * 2 + to % 2
        piece = orbitals_ref.at[:, group * part : (group + 1) * part]
        cuts.append(pltpu.make_async_copy(piece, sent_ref.at[to], sems.at[to]))
    for cut in cuts:
        cut.start()
    pairs.wait()
    index = pairs_ref[...]
    place = lax.shift_right_logical(index, 5) * 16 + (index & 15)
    odd = (index & 16) > 0
    even_core = jnp.where((index >= 0) & ~odd, place, -1)
    odd_core = jnp.where((index >= 0) & odd, place, -1)
    where = jnp.concatenate([even_core, odd_core, even_core, odd_core], axis=0).astype(f32).astype(bf16)
    trials.wait()
    for block in range(slots_ref.shape[0]):
        lanes = slice(block * BLOCK, (block + 1) * BLOCK)
        slots_ref[block, :NB, :] = trials_ref[:, lanes]
        slots_ref[block, NB:ROWS, :] = where[:, lanes]
    for cut in cuts:
        cut.wait()


def prepare(orbitals, trial_vectors, pair_index):
    rows, points = orbitals.shape
    blocks = trial_vectors.shape[1] // BLOCK
    return pl.pallas_call(
        prepare_body,
        in_specs=[IN_HBM] * 3,
        out_specs=[IN_VMEM] * 2,
        out_shape=[
            pltpu.VMEM((16, rows, points // 4), bf16),
            pltpu.VMEM((blocks, ROWS, BLOCK), bf16),
        ],
        scratch_shapes=[
            pltpu.VMEM(trial_vectors.shape, bf16),
            pltpu.VMEM(pair_index.shape, jnp.int32),
            pltpu.SemaphoreType.DMA((16,)),
            pltpu.SemaphoreType.DMA((2,)),
        ],
        compiler_params=pltpu.CompilerParams(vmem_limit_bytes=LIMIT),
        name="prepare",
    )(*hbm(orbitals, trial_vectors, pair_index))


def density_body(
    group_ref,
    core_ref,
    mine_ref,
    other_ref,
    slots0_ref,
    slots1_ref,
    slots2_ref,
    slots3_ref,
    all_pot_ref,
    kept_ref,
    pot_ref,
    keep_ref,
    give_ref,
    list_ref,
    slots_ref,
    phit_ref,
    fieldt_ref,
    pieces_ref,
    dens_ref,
    sem,
    sems,
):
    points = phit_ref.shape[0]
    group = group_ref[0]
    fetch = pltpu.make_async_copy(all_pot_ref.at[:, pl.ds(group * points, points)], pot_ref, sem)
    fetch.start()
    each = slots0_ref.shape[0]
    for k, ref in enumerate((slots0_ref, slots1_ref, slots2_ref, slots3_ref)):
        slots_ref[pl.ds((group ^ k) * each, each)] = ref[...]
    half = mine_ref.shape[0]
    for core in range(2):

        @pl.when(core_ref[0] == core)
        def _():
            phit_ref[:, core * half : (core + 1) * half] = mine_ref[...].T
            phit_ref[:, (1 - core) * half : (2 - core) * half] = other_ref[...].T

    fieldt_ref[...] = jnp.zeros_like(fieldt_ref)
    blocks = slots_ref.shape[0]
    count = jnp.int32(0)
    for block in range(blocks):
        most = jnp.max(slots_ref[block, NB:ROWS, :].astype(f32))
        list_ref[1 + count] = jnp.int32(block)
        count += (most >= 0.0).astype(jnp.int32)
    list_ref[0] = count
    for extra in range(TAKE):
        list_ref[1 + count + extra] = jnp.int32(0)

    rows = lax.broadcasted_iota(jnp.int32, (half, TAKE * BLOCK), 0).astype(f32)

    def step(turn, unused):
        pieces, trials = [], []
        for k in range(TAKE):
            at = turn * TAKE + k
            block = list_ref[1 + at]
            where = slots_ref[block, NB:ROWS, :].astype(f32)
            pieces.append(jnp.where(at < count, where, -1.0))
            trials.append(slots_ref[block, :NB, :])
        where = jnp.concatenate(pieces, axis=1)
        trial = jnp.concatenate(trials, axis=1)

        def picked(row):
            even_core = (rows == where[row : row + 1]).astype(bf16)
            odd_core = (rows == where[row + 2 : row + 3]).astype(bf16)
            return dot(phit_ref[...], jnp.concatenate([even_core, odd_core], axis=0))

        dens = (picked(0) * picked(1)).astype(bf16)
        dens_ref[turn] = dens
        pltpu.make_async_copy(dens_ref.at[turn], kept_ref.at[turn], sems.at[turn]).start()
        fieldt_ref[...] += dot(dens, trial, NT)
        return unused

    turns = (count + TAKE - 1) // TAKE
    lax.fori_loop(0, turns, step, 0)
    fetch.wait()
    fieldt = fieldt_ref[...]
    upper = fieldt.astype(bf16)
    lower = (fieldt - upper.astype(f32)).astype(bf16)
    proj = folded(dot(pot_ref[...], jnp.concatenate([upper, lower], axis=1)).T).astype(bf16)
    width = keep_ref.shape[2]
    for piece in range(4):
        pieces_ref[piece] = proj[:, piece * width : (piece + 1) * width]
    core = core_ref[0]
    keep_ref[...] = pieces_ref[pl.ds(core * 2, 2)]
    give_ref[...] = pieces_ref[pl.ds((1 - core) * 2, 2)]

    def kept(turn, unused):
        pltpu.make_async_copy(dens_ref.at[turn], kept_ref.at[turn], sems.at[turn]).wait()
        return unused

    lax.fori_loop(0, turns, kept, 0)


def density(group, core, mine, other, slots, eigenpotentials):
    blocks = slots[0].shape[0] * len(slots)
    half, points = mine.shape
    neig = eigenpotentials.shape[0]
    turns = blocks // TAKE
    return pl.pallas_call(
        density_body,
        in_specs=[IN_SMEM] * 2 + [IN_VMEM] * 6 + [IN_HBM],
        out_specs=[IN_HBM, IN_VMEM, IN_VMEM, IN_VMEM, IN_SMEM],
        out_shape=[
            pltpu.HBM((turns, points, TAKE * BLOCK), bf16),
            pltpu.VMEM((neig, points), bf16),
            pltpu.VMEM((2, NB, neig // 4), bf16),
            pltpu.VMEM((2, NB, neig // 4), bf16),
            jax.ShapeDtypeStruct((1 + blocks + TAKE,), jnp.int32),
        ],
        scratch_shapes=[
            pltpu.VMEM((blocks, ROWS, BLOCK), bf16),
            pltpu.VMEM((points, 2 * half), bf16),
            pltpu.VMEM((points, NB), f32),
            pltpu.VMEM((4, NB, neig // 4), bf16),
            pltpu.VMEM((turns, points, TAKE * BLOCK), bf16),
            pltpu.SemaphoreType.DMA(()),
            pltpu.SemaphoreType.DMA((turns,)),
        ],
        compiler_params=pltpu.CompilerParams(vmem_limit_bytes=LIMIT),
        name="density",
    )(group, core, *vmem(mine, other, *slots), *hbm(eigenpotentials))


def direct_body(
    group_ref,
    core_ref,
    list_ref,
    mine_ref,
    other_ref,
    screening_ref,
    pot_ref,
    kept_ref,
    out0_ref,
    out1_ref,
    out2_ref,
    out3_ref,
    terms_ref,
    split_ref,
    dens_ref,
    sems,
):
    count = list_ref[0]
    turns = (count + TAKE - 1) // TAKE

    def fetch(turn, unused):
        pltpu.make_async_copy(kept_ref.at[turn], dens_ref.at[turn], sems.at[turn]).start()
        return unused

    lax.fori_loop(0, turns, fetch, 0)
    terms_ref[...] = jnp.zeros_like(terms_ref)
    half = mine_ref.shape[0] * mine_ref.shape[2]
    total = jnp.zeros((NB, pot_ref.shape[1]), f32)
    for ref, core in ((mine_ref, core_ref[0]), (other_ref, 1 - core_ref[0])):
        scales = jnp.where(core == 0, screening_ref[:, :half], screening_ref[:, half:])
        screened = jnp.concatenate([ref[0], ref[1]], axis=1) * scales
        rows = pot_ref[pl.ds(pl.multiple_of(core * half, half), half), :]
        total += folded(dot(in_two(screened), rows))
    split_ref[...] = in_two(total)
    each = out0_ref.shape[0]
    own = group_ref[0] * each

    def step(turn, unused):
        pltpu.make_async_copy(kept_ref.at[turn], dens_ref.at[turn], sems.at[turn]).wait()
        terms = folded(dot(split_ref[...], dens_ref[turn])).astype(bf16)
        for k in range(TAKE):
            at = turn * TAKE + k

            @pl.when(at < count)
            def _():
                terms_ref[list_ref[1 + at] ^ own] = terms[:, k * BLOCK : (k + 1) * BLOCK]

        return unused

    lax.fori_loop(0, turns, step, 0)
    for k, ref in enumerate((out0_ref, out1_ref, out2_ref, out3_ref)):
        ref[...] = terms_ref[k * each : (k + 1) * each]


def direct_terms(group, core, live, mine, other, screening, pot, dens):
    blocks = dens.shape[0] * TAKE
    return pl.pallas_call(
        direct_body,
        in_specs=[IN_SMEM] * 3 + [IN_VMEM] * 4 + [IN_HBM],
        out_specs=[IN_VMEM] * 4,
        out_shape=[pltpu.VMEM((blocks // 4, NB, BLOCK), bf16)] * 4,
        scratch_shapes=[
            pltpu.VMEM((blocks, NB, BLOCK), bf16),
            pltpu.VMEM((2 * NB, pot.shape[1]), bf16),
            pltpu.VMEM(dens.shape, bf16),
            pltpu.SemaphoreType.DMA((dens.shape[0],)),
        ],
        compiler_params=pltpu.CompilerParams(vmem_limit_bytes=LIMIT),
        name="direct_terms",
    )(group, core, live, *vmem(mine, other, screening, pot), *hbm(dens))


def shards(orbitals, eigenpotentials, screening, trial_vectors, pair_index):
    group = lax.axis_index(GROUP).astype(jnp.int32).reshape(1)
    core = lax.axis_index("c").astype(jnp.int32).reshape(1)
    scales = screening.reshape(1, -1)
    sent, own_slots = prepare(orbitals, trial_vectors, pair_index)
    slots = [own_slots]
    for k in range(1, 4):
        slots.append(lax.ppermute(own_slots, GROUP, [(i, i ^ k) for i in range(4)]))
    mine = exchange(sent, SOURCES)
    mine = mine.reshape(-1, mine.shape[2])
    other = lax.ppermute(mine, "c", [(0, 1), (1, 0)])
    dens, pot, keep, give, live = density(group, core, mine, other, slots, eigenpotentials)
    given = lax.ppermute(give, "c", [(0, 1), (1, 0)])
    half = (keep.astype(f32) + given.astype(f32)).astype(bf16)
    column = summed(exchange(copies(half, 4).reshape(8, *half.shape[1:]), COLUMN)).astype(bf16)
    wide = exchange(copies(column, 32), WIDE)
    part = jnp.sum(wide.reshape(2, 2, 8, *column.shape).astype(f32), axis=(0, 2))
    apart = lax.ppermute(part, "c", [(0, 1), (1, 0)])
    terms = direct_terms(group, core, live, part, apart, scales, pot, dens)
    owner = terms[0].astype(f32)
    for k in range(1, 4):
        owner += lax.ppermute(terms[k], GROUP, [(i, i ^ k) for i in range(4)]).astype(f32)
    owner = owner.astype(bf16)
    direct = summed(exchange(copies(owner, 8), SLAB))
    return direct.transpose(1, 0, 2).reshape(NB, -1)


def solution(mesh):
    fine = Mesh(mesh.devices.reshape(SIZES), AXES)
    return jax.shard_map(
        shards,
        mesh=fine,
        in_specs=(P(ORB, SLAB), P(None, SLAB), P(), P(None, ORB), P(None, ORB)),
        out_specs=P(None, ORB),
        check_vma=False,
    )
```

```python
import jax
import jax.numpy as jnp
from jax import lax
from jax.experimental import pallas as pl
from jax.experimental.pallas import tpu as pltpu
from jax.sharding import Mesh, PartitionSpec as P


AXES = ("yl", "zh", "zl", "c", "yh", "x")
SIZES = (2, 4, 2, 2, 2, 4)
ORB = ("yl", "zh", "zl", "c")
SLAB = ("yh", "x")
GROUP = ("yl", "zl")
SOURCES = ("yl", "zh", "zl")
COLUMN = ("zh", "zl", "c")
WIDE = ("yl", "zl", "yh", "x")

NB = 16
BLOCK = 128
ROWS = 24
TAKE = 4

f32 = jnp.float32
bf16 = jnp.bfloat16
NT = (((1,), (1,)), ((), ()))
LIMIT = 30 * 1024 * 1024


def exchange(blocks, axes):
    return lax.all_to_all(blocks, axes, 0, 0, tiled=True)


def summed(blocks):
    return jnp.sum(blocks.astype(f32), axis=0)


def copies(value, count):
    return jnp.broadcast_to(value[None], (count, *value.shape))


def in_two(value):
    upper = value.astype(bf16)
    lower = (value - upper.astype(f32)).astype(bf16)
    return jnp.concatenate([upper, lower], axis=0)


def folded(both):
    return both[:NB] + both[NB:]


def dot(left, right, dims=(((1,), (0,)), ((), ()))):
    return lax.dot_general(left, right, dims, preferred_element_type=f32)


def vmem(*values):
    return [pltpu.with_memory_space_constraint(v, pltpu.VMEM) for v in values]


def hbm(*values):
    return [pltpu.with_memory_space_constraint(v, pltpu.HBM) for v in values]


IN_VMEM = pl.BlockSpec(memory_space=pltpu.VMEM)
IN_SMEM = pl.BlockSpec(memory_space=pltpu.SMEM)
IN_HBM = pl.BlockSpec(memory_space=pltpu.HBM)


def prepare_body(orbitals_ref, trial_ref, pair_ref, sent_ref, slots_ref, trials_ref, pairs_ref, sems, in_sems):
    part = sent_ref.shape[2]
    trials = pltpu.make_async_copy(trial_ref, trials_ref, in_sems.at[0])
    pairs = pltpu.make_async_copy(pair_ref, pairs_ref, in_sems.at[1])
    pairs.start()
    trials.start()
    cuts = []
    for to in range(sent_ref.shape[0]):
        group = (to // 8) * 2 + to % 2
        piece = orbitals_ref.at[:, group * part : (group + 1) * part]
        cuts.append(pltpu.make_async_copy(piece, sent_ref.at[to], sems.at[to]))
    for cut in cuts:
        cut.start()
    pairs.wait()
    index = pairs_ref[...]
    place = lax.shift_right_logical(index, 5) * 16 + (index & 15)
    odd = (index & 16) > 0
    even_core = jnp.where((index >= 0) & ~odd, place, -1)
    odd_core = jnp.where((index >= 0) & odd, place, -1)
    where = jnp.concatenate([even_core, odd_core, even_core, odd_core], axis=0).astype(f32).astype(bf16)
    trials.wait()
    for block in range(slots_ref.shape[0]):
        lanes = slice(block * BLOCK, (block + 1) * BLOCK)
        slots_ref[block, :NB, :] = trials_ref[:, lanes]
        slots_ref[block, NB:ROWS, :] = where[:, lanes]
    for cut in cuts:
        cut.wait()


def prepare(orbitals, trial_vectors, pair_index):
    rows, points = orbitals.shape
    blocks = trial_vectors.shape[1] // BLOCK
    return pl.pallas_call(
        prepare_body,
        in_specs=[IN_HBM] * 3,
        out_specs=[IN_VMEM] * 2,
        out_shape=[
            pltpu.VMEM((16, rows, points // 4), bf16),
            pltpu.VMEM((blocks, ROWS, BLOCK), bf16),
        ],
        scratch_shapes=[
            pltpu.VMEM(trial_vectors.shape, bf16),
            pltpu.VMEM(pair_index.shape, jnp.int32),
            pltpu.SemaphoreType.DMA((16,)),
            pltpu.SemaphoreType.DMA((2,)),
        ],
        compiler_params=pltpu.CompilerParams(vmem_limit_bytes=LIMIT),
        name="prepare",
    )(*hbm(orbitals, trial_vectors, pair_index))


def density_body(
    group_ref,
    core_ref,
    mine_ref,
    other_ref,
    slots0_ref,
    slots1_ref,
    slots2_ref,
    slots3_ref,
    all_pot_ref,
    kept_ref,
    pot_ref,
    quarters_ref,
    list_ref,
    slots_ref,
    phit_ref,
    field_ref,
    dens_ref,
    sem,
    sems,
):
    points = phit_ref.shape[0]
    group = group_ref[0]
    fetch = pltpu.make_async_copy(all_pot_ref.at[:, pl.ds(group * points, points)], pot_ref, sem)
    fetch.start()
    each = slots0_ref.shape[0]
    for k, ref in enumerate((slots0_ref, slots1_ref, slots2_ref, slots3_ref)):
        slots_ref[pl.ds((group ^ k) * each, each)] = ref[...]
    half = mine_ref.shape[0]
    for core in range(2):

        @pl.when(core_ref[0] == core)
        def _():
            phit_ref[:, core * half : (core + 1) * half] = mine_ref[...].T
            phit_ref[:, (1 - core) * half : (2 - core) * half] = other_ref[...].T

    field_ref[...] = jnp.zeros_like(field_ref)
    blocks = slots_ref.shape[0]
    count = jnp.int32(0)
    for block in range(blocks):
        most = jnp.max(slots_ref[block, NB:ROWS, :].astype(f32))
        list_ref[1 + count] = jnp.int32(block)
        count += (most >= 0.0).astype(jnp.int32)
    list_ref[0] = count
    for extra in range(TAKE):
        list_ref[1 + count + extra] = jnp.int32(0)

    rows = lax.broadcasted_iota(jnp.int32, (half, TAKE * BLOCK), 0).astype(f32)

    def step(turn, unused):
        pieces, trials = [], []
        for k in range(TAKE):
            at = turn * TAKE + k
            block = list_ref[1 + at]
            where = slots_ref[block, NB:ROWS, :].astype(f32)
            pieces.append(jnp.where(at < count, where, -1.0))
            trials.append(slots_ref[block, :NB, :])
        where = jnp.concatenate(pieces, axis=1)
        trial = jnp.concatenate(trials, axis=1)

        def picked(row):
            even_core = (rows == where[row : row + 1]).astype(bf16)
            odd_core = (rows == where[row + 2 : row + 3]).astype(bf16)
            return dot(phit_ref[...], jnp.concatenate([even_core, odd_core], axis=0))

        dens = (picked(0) * picked(1)).astype(bf16)
        dens_ref[turn] = dens
        pltpu.make_async_copy(dens_ref.at[turn], kept_ref.at[turn], sems.at[turn]).start()
        field_ref[...] += dot(trial, dens, NT)
        return unused

    turns = (count + TAKE - 1) // TAKE
    lax.fori_loop(0, turns, step, 0)
    fetch.wait()
    fieldt = field_ref[...].T
    upper = fieldt.astype(bf16)
    lower = (fieldt - upper.astype(f32)).astype(bf16)
    proj = folded(dot(pot_ref[...], jnp.concatenate([upper, lower], axis=1)).T).astype(bf16)
    width = quarters_ref.shape[2]
    for to in range(16):
        quarter = (to % 2) * 2 + (to // 2) % 2
        quarters_ref[to] = proj[:, quarter * width : (quarter + 1) * width]

    def kept(turn, unused):
        pltpu.make_async_copy(dens_ref.at[turn], kept_ref.at[turn], sems.at[turn]).wait()
        return unused

    lax.fori_loop(0, turns, kept, 0)


def density(group, core, mine, other, slots, eigenpotentials):
    blocks = slots[0].shape[0] * len(slots)
    half, points = mine.shape
    neig = eigenpotentials.shape[0]
    turns = blocks // TAKE
    return pl.pallas_call(
        density_body,
        in_specs=[IN_SMEM] * 2 + [IN_VMEM] * 6 + [IN_HBM],
        out_specs=[IN_HBM, IN_VMEM, IN_VMEM, IN_SMEM],
        out_shape=[
            pltpu.HBM((turns, points, TAKE * BLOCK), bf16),
            pltpu.VMEM((neig, points), bf16),
            pltpu.VMEM((16, NB, neig // 4), bf16),
            jax.ShapeDtypeStruct((1 + blocks + TAKE,), jnp.int32),
        ],
        scratch_shapes=[
            pltpu.VMEM((blocks, ROWS, BLOCK), bf16),
            pltpu.VMEM((points, 2 * half), bf16),
            pltpu.VMEM((NB, points), f32),
            pltpu.VMEM((turns, points, TAKE * BLOCK), bf16),
            pltpu.SemaphoreType.DMA(()),
            pltpu.SemaphoreType.DMA((turns,)),
        ],
        compiler_params=pltpu.CompilerParams(vmem_limit_bytes=LIMIT),
        name="density",
    )(group, core, *vmem(mine, other, *slots), *hbm(eigenpotentials))


def direct_body(
    group_ref,
    core_ref,
    list_ref,
    mine_ref,
    other_ref,
    screening_ref,
    pot_ref,
    kept_ref,
    out0_ref,
    out1_ref,
    out2_ref,
    out3_ref,
    terms_ref,
    split_ref,
    dens_ref,
    sems,
):
    count = list_ref[0]
    turns = (count + TAKE - 1) // TAKE

    def fetch(turn, unused):
        pltpu.make_async_copy(kept_ref.at[turn], dens_ref.at[turn], sems.at[turn]).start()
        return unused

    lax.fori_loop(0, turns, fetch, 0)
    terms_ref[...] = jnp.zeros_like(terms_ref)
    half = mine_ref.shape[0] * mine_ref.shape[2]
    total = jnp.zeros((NB, pot_ref.shape[1]), f32)
    for ref, core in ((mine_ref, core_ref[0]), (other_ref, 1 - core_ref[0])):
        scales = jnp.where(core == 0, screening_ref[:, :half], screening_ref[:, half:])
        screened = jnp.concatenate([ref[0], ref[1]], axis=1) * scales
        rows = pot_ref[pl.ds(pl.multiple_of(core * half, half), half), :]
        total += folded(dot(in_two(screened), rows))
    split_ref[...] = in_two(total)
    each = out0_ref.shape[0]
    own = group_ref[0] * each

    def step(turn, unused):
        pltpu.make_async_copy(kept_ref.at[turn], dens_ref.at[turn], sems.at[turn]).wait()
        terms = folded(dot(split_ref[...], dens_ref[turn])).astype(bf16)
        for k in range(TAKE):
            at = turn * TAKE + k

            @pl.when(at < count)
            def _():
                terms_ref[list_ref[1 + at] ^ own] = terms[:, k * BLOCK : (k + 1) * BLOCK]

        return unused

    lax.fori_loop(0, turns, step, 0)
    for k, ref in enumerate((out0_ref, out1_ref, out2_ref, out3_ref)):
        ref[...] = terms_ref[k * each : (k + 1) * each]


def direct_terms(group, core, live, mine, other, screening, pot, dens):
    blocks = dens.shape[0] * TAKE
    return pl.pallas_call(
        direct_body,
        in_specs=[IN_SMEM] * 3 + [IN_VMEM] * 4 + [IN_HBM],
        out_specs=[IN_VMEM] * 4,
        out_shape=[pltpu.VMEM((blocks // 4, NB, BLOCK), bf16)] * 4,
        scratch_shapes=[
            pltpu.VMEM((blocks, NB, BLOCK), bf16),
            pltpu.VMEM((2 * NB, pot.shape[1]), bf16),
            pltpu.VMEM(dens.shape, bf16),
            pltpu.SemaphoreType.DMA((dens.shape[0],)),
        ],
        compiler_params=pltpu.CompilerParams(vmem_limit_bytes=LIMIT),
        name="direct_terms",
    )(group, core, live, *vmem(mine, other, screening, pot), *hbm(dens))


def shards(orbitals, eigenpotentials, screening, trial_vectors, pair_index):
    group = lax.axis_index(GROUP).astype(jnp.int32).reshape(1)
    core = lax.axis_index("c").astype(jnp.int32).reshape(1)
    scales = screening.reshape(1, -1)
    sent, own_slots = prepare(orbitals, trial_vectors, pair_index)
    slots = [own_slots]
    for k in range(1, 4):
        slots.append(lax.ppermute(own_slots, GROUP, [(i, i ^ k) for i in range(4)]))
    mine = exchange(sent, SOURCES)
    mine = mine.reshape(-1, mine.shape[2])
    other = lax.ppermute(mine, "c", [(0, 1), (1, 0)])
    dens, pot, quarters, live = density(group, core, mine, other, slots, eigenpotentials)
    column = summed(exchange(quarters, COLUMN)).astype(bf16)
    wide = exchange(copies(column, 32), WIDE)
    part = jnp.sum(wide.reshape(2, 2, 8, *column.shape).astype(f32), axis=(0, 2))
    apart = lax.ppermute(part, "c", [(0, 1), (1, 0)])
    terms = direct_terms(group, core, live, part, apart, scales, pot, dens)
    owner = terms[0].astype(f32)
    for k in range(1, 4):
        owner += lax.ppermute(terms[k], GROUP, [(i, i ^ k) for i in range(4)]).astype(f32)
    owner = owner.astype(bf16)
    direct = summed(exchange(copies(owner, 8), SLAB))
    return direct.transpose(1, 0, 2).reshape(NB, -1)


def solution(mesh):
    fine = Mesh(mesh.devices.reshape(SIZES), AXES)
    return jax.shard_map(
        shards,
        mesh=fine,
        in_specs=(P(ORB, SLAB), P(None, SLAB), P(), P(None, ORB), P(None, ORB)),
        out_specs=P(None, ORB),
        check_vma=False,
    )
```

```python
import jax
import jax.numpy as jnp
from jax import lax
from jax.experimental import pallas as pl
from jax.experimental.pallas import tpu as pltpu
from jax.sharding import Mesh, PartitionSpec as P


AXES = ("yl", "zh", "zl", "c", "yh", "x")
SIZES = (2, 4, 2, 2, 2, 4)
ORB = ("yl", "zh", "zl", "c")
SLAB = ("yh", "x")
GROUP = ("yl", "zl")
SOURCES = ("yl", "zh", "zl")
COLUMN = ("zh", "zl", "c")
WIDE = ("yl", "zl", "yh", "x")

NB = 16
BLOCK = 128
ROWS = 24
TAKE = 2

f32 = jnp.float32
bf16 = jnp.bfloat16
NT = (((1,), (1,)), ((), ()))
LIMIT = 30 * 1024 * 1024


def exchange(blocks, axes):
    return lax.all_to_all(blocks, axes, 0, 0, tiled=True)


def summed(blocks):
    return jnp.sum(blocks.astype(f32), axis=0)


def copies(value, count):
    return jnp.broadcast_to(value[None], (count, *value.shape))


def in_two(value):
    upper = value.astype(bf16)
    lower = (value - upper.astype(f32)).astype(bf16)
    return jnp.concatenate([upper, lower], axis=0)


def folded(both):
    return both[:NB] + both[NB:]


def dot(left, right, dims=(((1,), (0,)), ((), ()))):
    return lax.dot_general(left, right, dims, preferred_element_type=f32)


def vmem(*values):
    return [pltpu.with_memory_space_constraint(v, pltpu.VMEM) for v in values]


def hbm(*values):
    return [pltpu.with_memory_space_constraint(v, pltpu.HBM) for v in values]


IN_VMEM = pl.BlockSpec(memory_space=pltpu.VMEM)
IN_SMEM = pl.BlockSpec(memory_space=pltpu.SMEM)
IN_HBM = pl.BlockSpec(memory_space=pltpu.HBM)


def prepare_body(orbitals_ref, trial_ref, pair_ref, sent_ref, slots_ref, trials_ref, pairs_ref, sems, in_sems):
    part = sent_ref.shape[2]
    trials = pltpu.make_async_copy(trial_ref, trials_ref, in_sems.at[0])
    pairs = pltpu.make_async_copy(pair_ref, pairs_ref, in_sems.at[1])
    pairs.start()
    trials.start()
    cuts = []
    for to in range(sent_ref.shape[0]):
        group = (to // 8) * 2 + to % 2
        piece = orbitals_ref.at[:, group * part : (group + 1) * part]
        cuts.append(pltpu.make_async_copy(piece, sent_ref.at[to], sems.at[to]))
    for cut in cuts:
        cut.start()
    pairs.wait()
    index = pairs_ref[...]
    place = lax.shift_right_logical(index, 5) * 16 + (index & 15)
    odd = (index & 16) > 0
    even_core = jnp.where((index >= 0) & ~odd, place, -1)
    odd_core = jnp.where((index >= 0) & odd, place, -1)
    where = jnp.concatenate([even_core, odd_core, even_core, odd_core], axis=0).astype(f32).astype(bf16)
    trials.wait()
    for block in range(slots_ref.shape[0]):
        lanes = slice(block * BLOCK, (block + 1) * BLOCK)
        slots_ref[block, :NB, :] = trials_ref[:, lanes]
        slots_ref[block, NB:ROWS, :] = where[:, lanes]
    for cut in cuts:
        cut.wait()


def prepare(orbitals, trial_vectors, pair_index):
    rows, points = orbitals.shape
    blocks = trial_vectors.shape[1] // BLOCK
    return pl.pallas_call(
        prepare_body,
        in_specs=[IN_HBM] * 3,
        out_specs=[IN_VMEM] * 2,
        out_shape=[
            pltpu.VMEM((16, rows, points // 4), bf16),
            pltpu.VMEM((blocks, ROWS, BLOCK), bf16),
        ],
        scratch_shapes=[
            pltpu.VMEM(trial_vectors.shape, bf16),
            pltpu.VMEM(pair_index.shape, jnp.int32),
            pltpu.SemaphoreType.DMA((16,)),
            pltpu.SemaphoreType.DMA((2,)),
        ],
        compiler_params=pltpu.CompilerParams(vmem_limit_bytes=LIMIT),
        name="prepare",
    )(*hbm(orbitals, trial_vectors, pair_index))


def density_body(
    group_ref,
    core_ref,
    mine_ref,
    other_ref,
    slots0_ref,
    slots1_ref,
    slots2_ref,
    slots3_ref,
    all_pot_ref,
    kept_ref,
    pot_ref,
    quarters_ref,
    list_ref,
    slots_ref,
    phit_ref,
    field_ref,
    dens_ref,
    sem,
    sems,
):
    points = phit_ref.shape[0]
    group = group_ref[0]
    fetch = pltpu.make_async_copy(all_pot_ref.at[:, pl.ds(group * points, points)], pot_ref, sem)
    fetch.start()
    each = slots0_ref.shape[0]
    for k, ref in enumerate((slots0_ref, slots1_ref, slots2_ref, slots3_ref)):
        slots_ref[pl.ds((group ^ k) * each, each)] = ref[...]
    half = mine_ref.shape[0]
    for core in range(2):

        @pl.when(core_ref[0] == core)
        def _():
            phit_ref[:, core * half : (core + 1) * half] = mine_ref[...].T
            phit_ref[:, (1 - core) * half : (2 - core) * half] = other_ref[...].T

    field_ref[...] = jnp.zeros_like(field_ref)
    blocks = slots_ref.shape[0]
    count = jnp.int32(0)
    for block in range(blocks):
        most = jnp.max(slots_ref[block, NB:ROWS, :].astype(f32))
        list_ref[1 + count] = jnp.int32(block)
        count += (most >= 0.0).astype(jnp.int32)
    list_ref[0] = count
    for extra in range(TAKE):
        list_ref[1 + count + extra] = jnp.int32(0)

    rows = lax.broadcasted_iota(jnp.int32, (half, TAKE * BLOCK), 0).astype(f32).astype(bf16)
    one, none = jnp.ones((), bf16), jnp.zeros((), bf16)

    def step(turn, unused):
        pieces, trials = [], []
        for k in range(TAKE):
            at = turn * TAKE + k
            block = list_ref[1 + at]
            where = slots_ref[block, NB:ROWS, :].astype(f32)
            pieces.append(jnp.where(at < count, where, -1.0))
            trials.append(slots_ref[block, :NB, :])
        where = jnp.concatenate(pieces, axis=1).astype(bf16)
        trial = jnp.concatenate(trials, axis=1)

        def picked(row):
            even_core = jnp.where(rows == where[row : row + 1], one, none)
            odd_core = jnp.where(rows == where[row + 2 : row + 3], one, none)
            return dot(phit_ref[...], jnp.concatenate([even_core, odd_core], axis=0))

        dens = picked(0).astype(bf16) * picked(1).astype(bf16)
        dens_ref[turn] = dens
        pltpu.make_async_copy(dens_ref.at[turn], kept_ref.at[turn], sems.at[turn]).start()
        field_ref[...] += dot(trial, dens, NT)
        return unused

    turns = (count + TAKE - 1) // TAKE
    lax.fori_loop(0, turns, step, 0)
    fetch.wait()
    fieldt = field_ref[...].T
    upper = fieldt.astype(bf16)
    lower = (fieldt - upper.astype(f32)).astype(bf16)
    proj = folded(dot(pot_ref[...], jnp.concatenate([upper, lower], axis=1)).T).astype(bf16)
    width = quarters_ref.shape[2]
    for to in range(16):
        quarter = (to % 2) * 2 + (to // 2) % 2
        quarters_ref[to] = proj[:, quarter * width : (quarter + 1) * width]

    def kept(turn, unused):
        pltpu.make_async_copy(dens_ref.at[turn], kept_ref.at[turn], sems.at[turn]).wait()
        return unused

    lax.fori_loop(0, turns, kept, 0)


def density(group, core, mine, other, slots, eigenpotentials):
    blocks = slots[0].shape[0] * len(slots)
    half, points = mine.shape
    neig = eigenpotentials.shape[0]
    turns = blocks // TAKE
    return pl.pallas_call(
        density_body,
        in_specs=[IN_SMEM] * 2 + [IN_VMEM] * 6 + [IN_HBM],
        out_specs=[IN_HBM, IN_VMEM, IN_VMEM, IN_SMEM],
        out_shape=[
            pltpu.HBM((turns, points, TAKE * BLOCK), bf16),
            pltpu.VMEM((neig, points), bf16),
            pltpu.VMEM((16, NB, neig // 4), bf16),
            jax.ShapeDtypeStruct((1 + blocks + TAKE,), jnp.int32),
        ],
        scratch_shapes=[
            pltpu.VMEM((blocks, ROWS, BLOCK), bf16),
            pltpu.VMEM((points, 2 * half), bf16),
            pltpu.VMEM((NB, points), f32),
            pltpu.VMEM((turns, points, TAKE * BLOCK), bf16),
            pltpu.SemaphoreType.DMA(()),
            pltpu.SemaphoreType.DMA((turns,)),
        ],
        compiler_params=pltpu.CompilerParams(vmem_limit_bytes=LIMIT),
        name="density",
    )(group, core, *vmem(mine, other, *slots), *hbm(eigenpotentials))


def direct_body(
    group_ref,
    core_ref,
    list_ref,
    mine_ref,
    other_ref,
    screening_ref,
    pot_ref,
    kept_ref,
    out0_ref,
    out1_ref,
    out2_ref,
    out3_ref,
    terms_ref,
    split_ref,
    dens_ref,
    sems,
):
    count = list_ref[0]
    turns = (count + TAKE - 1) // TAKE

    def fetch(turn, unused):
        pltpu.make_async_copy(kept_ref.at[turn], dens_ref.at[turn], sems.at[turn]).start()
        return unused

    lax.fori_loop(0, turns, fetch, 0)
    terms_ref[...] = jnp.zeros_like(terms_ref)
    half = mine_ref.shape[0] * mine_ref.shape[2]
    total = jnp.zeros((NB, pot_ref.shape[1]), f32)
    for ref, core in ((mine_ref, core_ref[0]), (other_ref, 1 - core_ref[0])):
        scales = jnp.where(core == 0, screening_ref[:, :half], screening_ref[:, half:])
        screened = jnp.concatenate([ref[0], ref[1]], axis=1) * scales
        rows = pot_ref[pl.ds(pl.multiple_of(core * half, half), half), :]
        total += folded(dot(in_two(screened), rows))
    split_ref[...] = in_two(total)
    each = out0_ref.shape[0]
    own = group_ref[0] * each

    def step(turn, unused):
        pltpu.make_async_copy(kept_ref.at[turn], dens_ref.at[turn], sems.at[turn]).wait()
        terms = folded(dot(split_ref[...], dens_ref[turn])).astype(bf16)
        for k in range(TAKE):
            at = turn * TAKE + k

            @pl.when(at < count)
            def _():
                terms_ref[list_ref[1 + at] ^ own] = terms[:, k * BLOCK : (k + 1) * BLOCK]

        return unused

    lax.fori_loop(0, turns, step, 0)
    for k, ref in enumerate((out0_ref, out1_ref, out2_ref, out3_ref)):
        ref[...] = terms_ref[k * each : (k + 1) * each]


def direct_terms(group, core, live, mine, other, screening, pot, dens):
    blocks = dens.shape[0] * TAKE
    return pl.pallas_call(
        direct_body,
        in_specs=[IN_SMEM] * 3 + [IN_VMEM] * 4 + [IN_HBM],
        out_specs=[IN_VMEM] * 4,
        out_shape=[pltpu.VMEM((blocks // 4, NB, BLOCK), bf16)] * 4,
        scratch_shapes=[
            pltpu.VMEM((blocks, NB, BLOCK), bf16),
            pltpu.VMEM((2 * NB, pot.shape[1]), bf16),
            pltpu.VMEM(dens.shape, bf16),
            pltpu.SemaphoreType.DMA((dens.shape[0],)),
        ],
        compiler_params=pltpu.CompilerParams(vmem_limit_bytes=LIMIT),
        name="direct_terms",
    )(group, core, live, *vmem(mine, other, screening, pot), *hbm(dens))


def shards(orbitals, eigenpotentials, screening, trial_vectors, pair_index):
    group = lax.axis_index(GROUP).astype(jnp.int32).reshape(1)
    core = lax.axis_index("c").astype(jnp.int32).reshape(1)
    scales = screening.reshape(1, -1)
    sent, own_slots = prepare(orbitals, trial_vectors, pair_index)
    slots = [own_slots]
    for k in range(1, 4):
        slots.append(lax.ppermute(own_slots, GROUP, [(i, i ^ k) for i in range(4)]))
    mine = exchange(sent, SOURCES)
    mine = mine.reshape(-1, mine.shape[2])
    other = lax.ppermute(mine, "c", [(0, 1), (1, 0)])
    dens, pot, quarters, live = density(group, core, mine, other, slots, eigenpotentials)
    column = summed(exchange(quarters, COLUMN)).astype(bf16)
    wide = exchange(copies(column, 32), WIDE)
    part = jnp.sum(wide.reshape(2, 2, 8, *column.shape).astype(f32), axis=(0, 2))
    apart = lax.ppermute(part, "c", [(0, 1), (1, 0)])
    terms = direct_terms(group, core, live, part, apart, scales, pot, dens)
    owner = terms[0].astype(f32)
    for k in range(1, 4):
        owner += lax.ppermute(terms[k], GROUP, [(i, i ^ k) for i in range(4)]).astype(f32)
    owner = owner.astype(bf16)
    direct = summed(exchange(copies(owner, 8), SLAB))
    return direct.transpose(1, 0, 2).reshape(NB, -1)


def solution(mesh):
    fine = Mesh(mesh.devices.reshape(SIZES), AXES)
    return jax.shard_map(
        shards,
        mesh=fine,
        in_specs=(P(ORB, SLAB), P(None, SLAB), P(), P(None, ORB), P(None, ORB)),
        out_specs=P(None, ORB),
        check_vma=False,
    )
```
